128 devices in a mesh: tile: 8 (over y, core), slab: 16 (over z, x).
Axes of the slice: x: 4, y: 4, z: 4, core: 2. Of those that a mesh axis runs over, the one named last changes fastest.
Arguments:
- volume: float32 [512, 32768], P('slab', 'tile'), may hold values from -6 to 6
- measured: float32 [512, 8192], P('slab', 'tile'), may hold values from -6 to 6
- weights: float32 [512, 8192], P('slab', 'tile'), may hold values from 0.25 to 4
- footprints: float32 [2048, 32, 128], P('tile'), may hold values from -0.1875 to 0.1875
- foot_pixel: int32 [2048], P('tile'), may hold values from 0 to 31
- foot_strip: int32 [2048], P('tile'), may hold values from 0 to 255
Outputs:
- smoothed: float32 [512, 32768], P('slab', 'tile')
- residual: float32 [512, 8192], P('slab', 'tile')
The draws below stay inside these ranges and needn't reach their ends.
Inputs may be any that keep to these rules, and one draw needn't show every extreme that they name: foot_pixel names one of the 32 pixel blocks of the tile that holds the footprint block. foot_strip names a strip of 32 rays.
All inputs are finite; a program needn't handle non-finite values.
Results may differ from the reference program's by a relative error of at most 0.0003.
Values sent between devices are 32-bit elements; how exact they have to be, the bound alone decides.
No kernel may reach another device: no remote copies, remote signals or barrier semaphores. Data moves between devices by JAX's collectives and lax.ppermute only.
A program may use at most 64 MiB of HBM per device.

```python
import math
import jax
import jax.numpy as jnp
import numpy as np
from jax import lax

STEPS = 2
PASSES = 3
PB_DEV = 32
FB_DEV = 256
FOOT = 2048
PIX = 32768
SLICES = 512
RAYS = 8192
STRIPS = 256
N_TILE = 8


def with_ends(entries, key, smallest, largest):
    longest = entries.shape.index(max(entries.shape))
    spots = []
    for shift in (0, 1):
        where = [jax.random.randint(jax.random.fold_in(key, axis), (), 0, length) for axis, length in enumerate(entries.shape)]
        where[longest] = (where[longest] + shift) % entries.shape[longest]
        spots.append(tuple(where))
    return entries.at[spots[0]].set(smallest).at[spots[1]].set(largest)


def levels(rng, extent, cuts, low, high):
    gain, own = 1.0, jax.random.fold_in(rng, 6)
    for dim, parts in cuts:
        steps = jnp.exp(jax.random.uniform(jax.random.fold_in(own, dim), (parts,), jnp.float32, low / len(cuts), high / len(cuts)))
        gain = gain * jnp.repeat(steps, extent[dim] // parts).reshape([-1 if axis == dim else 1 for axis in range(len(extent))])
    return gain


def cumulative_ranks(count, lean):
    portions = [(1 << 20) // math.isqrt(grade ** lean) + 1 for grade in range(1, count + 1)]
    deviation = 1 + sum(portions) // (1 << 30)
    return np.cumsum(np.array([max(1, weight // deviation) for weight in portions]))


def ranked_ids(key, dims, number_of, skew):
    listing = cumulative_ranks(number_of, skew)
    lot = jax.random.randint(jax.random.fold_in(key, 1), dims, 0, int(listing[number_of - 1]))
    rank = jnp.searchsorted(jnp.asarray(listing, jnp.int32), lot, side="right")
    return jax.random.permutation(jax.random.fold_in(key, 2), number_of)[rank].astype(jnp.int32)


def normal_values(stream_key, extent, deviation, limit, split=(), kind=jnp.bfloat16):
    values = jax.random.normal(stream_key, extent, jnp.float32) * deviation
    if len(split) > 0:
        values = levels(stream_key, extent, split, -0.22, 0.18) * values
    return jnp.clip(values, min=-limit, max=limit).astype(kind)


def setup_inputs(seed: int = 0) -> dict:
    arg_keys = jax.random.split(jax.random.key(seed), 7)
    volume = normal_values(arg_keys[0], (SLICES, PIX), 1.0, 6.0, ((0, 16), (1, 8)), jnp.float32)
    measured = normal_values(arg_keys[1], (SLICES, RAYS), 1.0, 6.0, ((0, 16), (1, 8)), jnp.float32)
    weights = jnp.clip(jnp.exp(math.log(4.0) - 2.7725887 * jax.random.uniform(arg_keys[2], (SLICES, RAYS), jnp.float32) ** levels(arg_keys[2], (SLICES, RAYS), ((0, 16), (1, 8)), -0.2, 0.2)), 0.25, 4.0)
    footprints = normal_values(arg_keys[3], (FOOT, 32, 128), (128 * FOOT // STRIPS) ** -0.5, 0.1875, ((0, 8),), jnp.float32)
    foot_pixel = with_ends(jax.random.randint(arg_keys[4], (FOOT,), 0, PB_DEV), jax.random.fold_in(arg_keys[4], 1), 0, PB_DEV - 1).astype(jnp.int32)
    foot_strip = with_ends(ranked_ids(arg_keys[5], (FOOT,), STRIPS, 2), jax.random.fold_in(arg_keys[5], 3), 0, STRIPS - 1).astype(jnp.int32)
    return dict(volume=volume, measured=measured, weights=weights, footprints=footprints, foot_pixel=foot_pixel, foot_strip=foot_strip)


huber_width = 0.5
smooth_rate = 0.2
highest = lax.Precision.HIGHEST


def tile_project(blocked, blocks, pixel_ids, strip_ids):
    picked = jnp.take(blocked, pixel_ids, axis=1)
    contrib = jnp.einsum("sbj,bkj->sbk", picked, blocks, precision=highest)
    strip_hot = (strip_ids[:, None] == jnp.arange(STRIPS, dtype=jnp.int32)[None, :]).astype(jnp.float32)
    summed = jnp.einsum("sbk,bq->sqk", contrib, strip_hot, precision=highest)
    return summed.reshape(summed.shape[0], STRIPS * 32)


def tile_back(ray_values, blocks, pixel_ids, strip_ids, pixel_count):
    strip_rows = ray_values.reshape(ray_values.shape[0], STRIPS, 32)
    strip_hot = (strip_ids[:, None] == jnp.arange(STRIPS, dtype=jnp.int32)[None, :]).astype(jnp.float32)
    picked = jnp.einsum("sqk,bq->sbk", strip_rows, strip_hot, precision=highest)
    spread = jnp.einsum("sbk,bkj->sbj", picked, blocks, precision=highest)
    pixel_hot = (pixel_ids[:, None] == jnp.arange(pixel_count, dtype=jnp.int32)[None, :]).astype(jnp.float32)
    placed = jnp.einsum("sbj,bp->spj", spread, pixel_hot, precision=highest)
    return placed.reshape(ray_values.shape[0], pixel_count * 128)


def forward_all(field, footprints, foot_pixel, foot_strip):
    tiled = jnp.moveaxis(field.reshape(SLICES, N_TILE, PB_DEV, 128), 1, 0)
    blocks = footprints.reshape(N_TILE, FB_DEV, 32, 128)
    pixels = foot_pixel.reshape(N_TILE, FB_DEV)
    strips = foot_strip.reshape(N_TILE, FB_DEV)

    def add_tile(total, pieces):
        return total + tile_project(pieces[0], pieces[1], pieces[2], pieces[3]), None

    start_sum = jnp.zeros((SLICES, RAYS), jnp.float32)
    return lax.scan(add_tile, start_sum, (tiled, blocks, pixels, strips))[0]


def backward_all(ray_values, footprints, foot_pixel, foot_strip):
    blocks = footprints.reshape(N_TILE, FB_DEV, 32, 128)
    pixels = foot_pixel.reshape(N_TILE, FB_DEV)
    strips = foot_strip.reshape(N_TILE, FB_DEV)

    def one_tile(pieces):
        return tile_back(ray_values, pieces[0], pieces[1], pieces[2], PB_DEV)

    stacked = lax.map(one_tile, (blocks, pixels, strips))
    return jnp.moveaxis(stacked, 0, 1).reshape(SLICES, PIX)


def reference(volume, measured, weights, footprints, foot_pixel, foot_strip):
    residual = forward_all(volume, footprints, foot_pixel, foot_strip) - measured
    current = volume
    for number in range(STEPS):
        gradient = backward_all(weights * residual, footprints, foot_pixel, foot_strip)
        projected = forward_all(gradient, footprints, foot_pixel, foot_strip)
        grad_total = jnp.sum(gradient * gradient)
        curve_total = jnp.sum(weights * projected * projected)
        step_size = grad_total / curve_total
        current = current - step_size * gradient
        residual = residual - step_size * projected
    zero_row = jnp.zeros((1, current.shape[1]), jnp.float32)
    for number in range(PASSES):
        clipped = jnp.clip(current[1:] - current[:-1], -huber_width, huber_width)
        upper = jnp.concatenate([clipped, zero_row], axis=0)
        lower = jnp.concatenate([zero_row, clipped], axis=0)
        current = current + smooth_rate * (upper - lower)
    return current, residual
```

```python
import jax
import jax.numpy as jnp
from jax import lax
from jax.experimental import pallas as pl
from jax.experimental.pallas import tpu as pltpu
from jax.sharding import Mesh
from jax.sharding import PartitionSpec as P

PASSES = 3
TILE = ("tile_0", "tile_1")
SLAB = ("slab_0", "slab_1")
GROUP = 4

huber_width = 0.5
smooth_rate = 0.2


VM = pl.BlockSpec(memory_space=pltpu.VMEM)
SM = pl.BlockSpec(memory_space=pltpu.SMEM)
F32 = jnp.float32
BF16 = jnp.bfloat16


def call(kernel, outs, ins, scratch=(), smem=0, flops=1000000, limit=24):
    return pl.pallas_call(
        kernel,
        out_shape=[jax.ShapeDtypeStruct(s, F32) for s in outs],
        in_specs=[SM] * smem + [VM] * (len(ins) - smem),
        out_specs=[VM] * len(outs),
        scratch_shapes=list(scratch),
        compiler_params=pltpu.CompilerParams(vmem_limit_bytes=limit << 20),
        cost_estimate=pl.CostEstimate(flops=flops, bytes_accessed=1 << 20, transcendentals=0),
    )(*ins)


def halves(value):
    high = value.astype(BF16)
    return high, (value - high.astype(F32)).astype(BF16)


def lane_groups(shape):
    return lax.broadcasted_iota(jnp.int32, shape, 1) // 32


def place(meta, b):
    word = meta[b]
    return word & 63, (word >> 6) & 3, word >> 8


def forward_loop(meta, foot, high, low, rays):
    rays[...] = jnp.zeros_like(rays)
    groups = lane_groups((32, 128))

    def step(g, carry):
        where = [place(meta, GROUP * g + i) for i in range(GROUP)]
        left = jnp.concatenate([jnp.concatenate([high[w[2]], low[w[2]]], axis=1) for w in where], axis=0)
        fh, fl = halves(foot[pl.ds(GROUP * g, GROUP)].reshape(GROUP * 32, 128))
        right = jnp.concatenate(
            [jnp.concatenate([fh, fh], axis=1), jnp.concatenate([fl, jnp.zeros_like(fl)], axis=1)], axis=0
        )
        both = lax.dot_general(left, right, (((1,), (1,)), ((), ())), preferred_element_type=F32)
        product = both[:, :128] + both[:, 128:]
        for i, (entry, spot, _) in enumerate(where):
            own = jnp.where(groups == i, product[32 * i : 32 * i + 32], 0.0)
            rays[entry] += pltpu.roll(own, ((spot - i) & 3) * 32, 1)
        return carry

    lax.fori_loop(0, foot.shape[0] // GROUP, step, 0)


def back_loop(meta, foot, rays, field):
    field[...] = jnp.zeros_like(field)
    groups = lane_groups((32, 128))

    def step(g, carry):
        where = [place(meta, GROUP * g + i) for i in range(GROUP)]
        rows = []
        for i, (entry, spot, _) in enumerate(where):
            turned = pltpu.roll(rays[entry], ((i - spot) & 3) * 32, 1)
            own = jnp.where(groups == i, turned, 0.0)
            rows.append(jnp.concatenate(halves(own), axis=1))
        left = jnp.concatenate(rows, axis=0)
        fh, fl = halves(foot[pl.ds(GROUP * g, GROUP)].reshape(GROUP * 32, 128))
        right = jnp.concatenate(
            [jnp.concatenate([fh, fl], axis=1), jnp.concatenate([fh, jnp.zeros_like(fl)], axis=1)], axis=0
        )
        both = lax.dot_general(left, right, (((1,), (0,)), ((), ())), preferred_element_type=F32)
        product = both[:, :128] + both[:, 128:]
        for i, (_, _, pixel) in enumerate(where):
            field[pixel] += product[32 * i : 32 * i + 32]
        return carry

    lax.fori_loop(0, foot.shape[0] // GROUP, step, 0)


def hand_out(rays, mine, theirs):
    mine[...] = rays[:32].reshape(mine.shape)
    theirs[...] = rays[32:].reshape(theirs.shape)


def first_kernel(meta, foot, volume, mine, theirs, high, low, rays):
    for p in range(high.shape[0]):
        high[p], low[p] = halves(volume[:, 128 * p : 128 * p + 128])
    forward_loop(meta, foot, high, low, rays)
    hand_out(rays, mine, theirs)


def folded(value):
    return jnp.sum(value.reshape(-1, 8, 128), axis=0)


def there_and_back(meta, foot, pieces, mine, theirs, field, norm, high, low, rays):
    for slot, piece in enumerate(pieces):
        rays[8 * slot : 8 * slot + 8] = piece[...]
    back_loop(meta, foot, rays, field)
    for p in range(high.shape[0]):
        high[p], low[p] = halves(field[p])
    forward_loop(meta, foot, high, low, rays)
    hand_out(rays, mine, theirs)
    norm[...] = folded(field[...] * field[...])


def second_kernel(meta, foot, *refs):
    there_and_back(meta, foot, refs[:8], *refs[8:])


def third_kernel(meta, foot, *refs):
    pieces, volume, grad = refs[:8], refs[8], refs[9]
    mine, theirs, field, norm, first, last, high, low, rays = refs[10:]
    there_and_back(meta, foot, pieces, mine, theirs, field, norm, high, low, rays)
    for p in range(field.shape[0]):
        cols = slice(128 * p, 128 * p + 128)
        first[0, p], last[0, p] = volume[0:8, cols], volume[24:32, cols]
        first[1, p], last[1, p] = grad[p, 0:8], grad[p, 24:32]
        first[2, p], last[2, p] = field[p, 0:8], field[p, 24:32]


def add_kernel(mine, got, kept, s1, s2, s3):
    for r, out in enumerate((kept, s1, s2, s3)):
        out[...] = mine[r] + got[r]


def tile_cols(ref):
    return jnp.stack([ref[:, 128 * t : 128 * t + 128] for t in range(ref.shape[1] // 128)])


def start_kernel(kept, a, b, c, measured, weights, residual, sent):
    value = kept[...] + a[...] + b[...] + c[...] - tile_cols(measured)
    residual[...] = value
    sent[...] = tile_cols(weights) * value


def middle_kernel(kept, a, b, c, weights, norm, projected, sent, sums):
    value = kept[...] + a[...] + b[...] + c[...]
    weighted = tile_cols(weights) * value
    projected[...] = value
    sent[...] = weighted
    sums[0] = norm[...]
    sums[1] = folded(weighted * value)


def ratio(sums):
    return jnp.sum(sums[0], keepdims=True) / jnp.sum(sums[1], keepdims=True)


def end_kernel(kept, a, b, c, weights, before, grad, turned, sums, projected, out):
    alpha = ratio(sums)
    value = before[...] - alpha * (kept[...] + a[...] + b[...] + c[...])
    projected[...] = value
    step = grad[...] - alpha * turned[...]
    out[0] = folded(step * step)
    out[1] = folded(tile_cols(weights) * value * value)


def smooth_kernel(ends, volume, grad, turned, first, last, sums0, sums1, residual, p0, p1, smoothed, left_over):
    alpha0, alpha1 = ratio(sums0), ratio(sums1)
    rest = residual[...] - alpha0 * p0[...] - alpha1 * p1[...]
    for t in range(rest.shape[0]):
        left_over[:, 128 * t : 128 * t + 128] = rest[t]

    def stepped(x, g, h):
        return x - alpha0 * g - alpha1 * (g - alpha0 * h)

    row = lax.broadcasted_iota(jnp.int32, (48, 128), 0)
    open_link = ~(((row == 7) & (ends[0] == 1)) | ((row == 39) & (ends[1] == 1)))
    link = jnp.where(open_link, F32(1.0), F32(0.0))
    for p in range(grad.shape[0]):
        cols = slice(128 * p, 128 * p + 128)
        ext = jnp.concatenate(
            [
                stepped(last[0, p], last[1, p], last[2, p]),
                stepped(volume[:, cols], grad[p], turned[p]),
                stepped(first[0, p], first[1, p], first[2, p]),
            ],
            axis=0,
        )
        for _ in range(PASSES):
            clipped = jnp.clip(pltpu.roll(ext, 47, 0) - ext, -huber_width, huber_width) * link
            ext = ext + smooth_rate * (clipped - pltpu.roll(clipped, 1, 0))
        smoothed[:, cols] = ext[8:40]


def shift(value, axis, by):
    n = lax.axis_size(axis)
    return lax.ppermute(value, axis, [(i, (i + by) % n) for i in range(n)])


RAY = (8, 32, 128)


def summed_by_owner(mine, theirs):
    got = shift(theirs, "tile_1", 1)
    kept, s1, s2, s3 = call(add_kernel, [RAY] * 4, [mine, got])
    return kept, shift(s1, "tile_0", 1), shift(s2, "tile_0", 2), shift(s3, "tile_0", 3)


def to_everyone(own):
    column = [own] + [shift(own, "tile_0", -r) for r in (1, 2, 3)]
    return column + [shift(block, "tile_1", 1) for block in column]


def total(sums):
    for axis in ("tile_1", "tile_0", "slab_0", "slab_1"):
        sums = sums + sum(shift(sums, axis, r) for r in range(1, lax.axis_size(axis)))
    return sums


def shards(volume, measured, weights, footprints, foot_pixel, foot_strip):
    owner = foot_strip // 32
    core = (owner & 1) ^ lax.axis_index("tile_1")
    ahead = ((owner >> 1) - lax.axis_index("tile_0")) & 3
    meta = (core * 4 + ahead) * 8 + (foot_strip // 4) % 8 + (foot_strip % 4) * 64 + foot_pixel * 256

    half, field = (4,) + RAY, (32, 32, 128)
    scratch = [pltpu.VMEM(field, BF16), pltpu.VMEM(field, BF16), pltpu.VMEM((64, 32, 128), F32)]
    mine, theirs = call(first_kernel, [half, half], [meta, footprints, volume], scratch, 1)
    parts = summed_by_owner(mine, theirs)
    residual, sent = call(start_kernel, [RAY, RAY], [*parts, measured, weights])

    mine, theirs, grad, norm = call(
        second_kernel, [half, half, field, (8, 128)], [meta, footprints, *to_everyone(sent)], scratch, 1
    )
    parts = summed_by_owner(mine, theirs)
    p0, sent, sums0 = call(middle_kernel, [RAY, RAY, (2, 8, 128)], [*parts, weights, norm])

    edge = (3, 32, 8, 128)
    mine, theirs, turned, _, first, last = call(
        third_kernel,
        [half, half, field, (8, 128), edge, edge],
        [meta, footprints, *to_everyone(sent), volume, grad],
        scratch,
        1,
    )
    sums0 = total(sums0)
    slabs = lax.axis_size(SLAB)
    up = [(i, i + 1) for i in range(slabs - 1)]
    down = [(j, i) for i, j in up]
    last = lax.ppermute(last, SLAB, up)
    first = lax.ppermute(first, SLAB, down)
    parts = summed_by_owner(mine, theirs)
    p1, sums1 = call(end_kernel, [RAY, (2, 8, 128)], [*parts, weights, p0, grad, turned, sums0])
    sums1 = total(sums1)
    place_in = lax.axis_index(SLAB)
    ends = jnp.stack([place_in == 0, place_in == slabs - 1]).astype(jnp.int32)
    return call(
        smooth_kernel,
        [volume.shape, measured.shape],
        [ends, volume, grad, turned, first, last, sums0, sums1, residual, p0, p1],
        (),
        1,
    )


def solution(mesh):
    finer = Mesh(mesh.devices.reshape(4, 2, 4, 4), ("tile_0", "tile_1", "slab_0", "slab_1"))
    return jax.shard_map(
        lambda *args: tuple(shards(*args)),
        mesh=finer,
        in_specs=(
            P(SLAB, TILE),
            P(SLAB, TILE),
            P(SLAB, TILE),
            P(TILE, None, None),
            P(TILE),
            P(TILE),
        ),
        out_specs=(P(SLAB, TILE), P(SLAB, TILE)),
        check_vma=False,
    )
```

```python
import jax
import jax.numpy as jnp
from jax import lax
from jax.experimental import pallas as pl
from jax.experimental.pallas import tpu as pltpu
from jax.sharding import Mesh
from jax.sharding import PartitionSpec as P

PASSES = 3
TILE = ("tile_0", "tile_1")
SLAB = ("slab_0", "slab_1")
GROUP = 4
UNROLL = 16

huber_width = 0.5
smooth_rate = 0.2


VM = pl.BlockSpec(memory_space=pltpu.VMEM)
SM = pl.BlockSpec(memory_space=pltpu.SMEM)
F32 = jnp.float32
BF16 = jnp.bfloat16


def call(kernel, outs, ins, scratch=(), smem=0, flops=1000000, limit=24):
    return pl.pallas_call(
        kernel,
        out_shape=[jax.ShapeDtypeStruct(s, F32) for s in outs],
        in_specs=[SM] * smem + [VM] * (len(ins) - smem),
        out_specs=[VM] * len(outs),
        scratch_shapes=list(scratch),
        compiler_params=pltpu.CompilerParams(vmem_limit_bytes=limit << 20),
        cost_estimate=pl.CostEstimate(flops=flops, bytes_accessed=1 << 20, transcendentals=0),
    )(*ins)


def halves(value):
    high = value.astype(BF16)
    return high, (value - high.astype(F32)).astype(BF16)


def lane_groups(shape):
    return lax.broadcasted_iota(jnp.int32, shape, 1) // 32


def place(meta, b):
    word = meta[b]
    return word & 63, (word >> 6) & 3, word >> 8


def forward_loop(meta, foot, high, low, rays):
    rays[...] = jnp.zeros_like(rays)
    groups = lane_groups((32, 128))

    def step(g, carry):
        where = [place(meta, GROUP * g + i) for i in range(GROUP)]
        left = jnp.concatenate([jnp.concatenate([high[w[2]], low[w[2]]], axis=1) for w in where], axis=0)
        fh, fl = halves(foot[pl.ds(GROUP * g, GROUP)].reshape(GROUP * 32, 128))
        right = jnp.concatenate(
            [jnp.concatenate([fh, fh], axis=1), jnp.concatenate([fl, jnp.zeros_like(fl)], axis=1)], axis=0
        )
        both = lax.dot_general(left, right, (((1,), (1,)), ((), ())), preferred_element_type=F32)
        product = both[:, :128] + both[:, 128:]
        for i, (entry, spot, _) in enumerate(where):
            own = jnp.where(groups == i, product[32 * i : 32 * i + 32], 0.0)
            rays[entry] += pltpu.roll(own, ((spot - i) & 3) * 32, 1)
        return carry

    lax.fori_loop(0, foot.shape[0] // GROUP, step, 0, unroll=UNROLL)


def back_loop(meta, foot, rays, field):
    field[...] = jnp.zeros_like(field)
    groups = lane_groups((32, 128))

    def step(g, carry):
        where = [place(meta, GROUP * g + i) for i in range(GROUP)]
        rows = []
        for i, (entry, spot, _) in enumerate(where):
            turned = pltpu.roll(rays[entry], ((i - spot) & 3) * 32, 1)
            own = jnp.where(groups == i, turned, 0.0)
            rows.append(jnp.concatenate(halves(own), axis=1))
        left = jnp.concatenate(rows, axis=0)
        fh, fl = halves(foot[pl.ds(GROUP * g, GROUP)].reshape(GROUP * 32, 128))
        right = jnp.concatenate(
            [jnp.concatenate([fh, fl], axis=1), jnp.concatenate([fh, jnp.zeros_like(fl)], axis=1)], axis=0
        )
        both = lax.dot_general(left, right, (((1,), (0,)), ((), ())), preferred_element_type=F32)
        product = both[:, :128] + both[:, 128:]
        for i, (_, _, pixel) in enumerate(where):
            field[pixel] += product[32 * i : 32 * i + 32]
        return carry

    lax.fori_loop(0, foot.shape[0] // GROUP, step, 0, unroll=UNROLL)


def hand_out(rays, mine, theirs):
    mine[...] = rays[:32].reshape(mine.shape)
    theirs[...] = rays[32:].reshape(theirs.shape)


def first_kernel(meta, foot, volume, mine, theirs, high, low, rays):
    for p in range(high.shape[0]):
        high[p], low[p] = halves(volume[:, 128 * p : 128 * p + 128])
    forward_loop(meta, foot, high, low, rays)
    hand_out(rays, mine, theirs)


def folded(value):
    return jnp.sum(value.reshape(-1, 8, 128), axis=0)


def there_and_back(meta, foot, pieces, mine, theirs, field, high, low, rays):
    for slot, piece in enumerate(pieces):
        rays[8 * slot : 8 * slot + 8] = piece[...]
    back_loop(meta, foot, rays, field)
    for p in range(high.shape[0]):
        high[p], low[p] = halves(field[p])
    forward_loop(meta, foot, high, low, rays)
    hand_out(rays, mine, theirs)


def second_kernel(meta, foot, *refs):
    pieces, (mine, theirs, field, sums, high, low, rays) = refs[:8], refs[8:]
    there_and_back(meta, foot, pieces, mine, theirs, field, high, low, rays)
    sums[0] = folded(field[...] * field[...])


def third_kernel(meta, foot, *refs):
    pieces, volume, grad = refs[:8], refs[8], refs[9]
    mine, theirs, field, sums, first, last, high, low, rays = refs[10:]
    there_and_back(meta, foot, pieces, mine, theirs, field, high, low, rays)
    sums[0] = folded(grad[...] * field[...])
    sums[1] = folded(field[...] * field[...])
    for p in range(field.shape[0]):
        cols = slice(128 * p, 128 * p + 128)
        first[0, p], last[0, p] = volume[0:8, cols], volume[24:32, cols]
        first[1, p], last[1, p] = grad[p, 0:8], grad[p, 24:32]
        first[2, p], last[2, p] = field[p, 0:8], field[p, 24:32]


def add_kernel(mine, got, kept, s1, s2, s3):
    for r, out in enumerate((kept, s1, s2, s3)):
        out[...] = mine[r] + got[r]


def tile_cols(ref):
    return jnp.stack([ref[:, 128 * t : 128 * t + 128] for t in range(ref.shape[1] // 128)])


def start_kernel(kept, a, b, c, measured, weights, residual, sent):
    value = kept[...] + a[...] + b[...] + c[...] - tile_cols(measured)
    residual[...] = value
    sent[...] = tile_cols(weights) * value


def middle_kernel(kept, a, b, c, weights, projected, sent, sums):
    value = kept[...] + a[...] + b[...] + c[...]
    weighted = tile_cols(weights) * value
    projected[...] = value
    sent[...] = weighted
    sums[0] = folded(weighted * value)


def as_rows(sums, rows):
    lane = lax.broadcasted_iota(jnp.int32, rows.shape, 1)
    value = jnp.zeros(rows.shape, F32)
    for n, part in enumerate(sums):
        value = jnp.where(lane == n, jnp.sum(part, keepdims=True), value)
    rows[...] = value


def end_kernel(kept, a, b, c, weights, before, norm0, curve0, turned, projected, rows):
    value = kept[...] + a[...] + b[...] + c[...]
    weighted = tile_cols(weights) * value
    projected[...] = value
    cross = folded(weighted * before[...])
    as_rows([norm0[0], curve0[0], turned[0], turned[1], cross, folded(weighted * value)], rows)


def totals(rows, count):
    value = jnp.sum(rows[...], axis=0, keepdims=True)
    return [jnp.sum(value[:, n : n + 1]) for n in range(count)]


def judge_kernel(rows, alphas, again):
    norm0, curve0, cross_g, square_g, cross_p, square_p = totals(rows, 6)
    alpha = norm0 / curve0
    norm1 = norm0 - 2.0 * alpha * cross_g + alpha * alpha * square_g
    curve1 = curve0 - 2.0 * alpha * cross_p + alpha * alpha * square_p
    sound = (norm1 > 0.01 * norm0) & (curve1 > 0.01 * curve0)
    for square in (square_g, square_p):
        sound = sound & (square > 1e-25) & (square < 1e37)
    alphas[0] = alpha
    alphas[1] = norm1 / curve1
    again[0] = jnp.where(sound, 0, 1)


def again_kernel(alphas, weights, p0, q0, grad, turned, rows):
    value = p0[...] - alphas[0] * q0[...]
    step = grad[...] - alphas[0] * turned[...]
    as_rows([folded(step * step), folded(tile_cols(weights) * value * value)], rows)


def ratio_kernel(alphas, rows, out):
    norm1, curve1 = totals(rows, 2)
    out[0] = alphas[0]
    out[1] = norm1 / curve1


def smooth_kernel(ends, alphas, volume, grad, turned, first, last, residual, p0, q0, smoothed, left_over):
    alpha0, alpha1 = alphas[0], alphas[1]
    rest = residual[...] - alpha0 * p0[...] - alpha1 * (p0[...] - alpha0 * q0[...])
    for t in range(rest.shape[0]):
        left_over[:, 128 * t : 128 * t + 128] = rest[t]

    def stepped(x, g, h):
        return x - alpha0 * g - alpha1 * (g - alpha0 * h)

    row = lax.broadcasted_iota(jnp.int32, (48, 128), 0)
    open_link = ~(((row == 7) & (ends[0] == 1)) | ((row == 39) & (ends[1] == 1)))
    link = jnp.where(open_link, F32(1.0), F32(0.0))
    for p in range(grad.shape[0]):
        cols = slice(128 * p, 128 * p + 128)
        ext = jnp.concatenate(
            [
                stepped(last[0, p], last[1, p], last[2, p]),
                stepped(volume[:, cols], grad[p], turned[p]),
                stepped(first[0, p], first[1, p], first[2, p]),
            ],
            axis=0,
        )
        for _ in range(PASSES):
            clipped = jnp.clip(pltpu.roll(ext, 47, 0) - ext, -huber_width, huber_width) * link
            ext = ext + smooth_rate * (clipped - pltpu.roll(clipped, 1, 0))
        smoothed[:, cols] = ext[8:40]


def shift(value, axis, by):
    n = lax.axis_size(axis)
    return lax.ppermute(value, axis, [(i, (i + by) % n) for i in range(n)])


RAY = (8, 32, 128)


def summed_by_owner(mine, theirs):
    got = shift(theirs, "tile_1", 1)
    kept, s1, s2, s3 = call(add_kernel, [RAY] * 4, [mine, got])
    moved = []
    for r, part in enumerate((s1, s2, s3), 1):
        moved.append(shift(part, "tile_0", r))
    return kept, *moved


def to_everyone(own):
    column = [own] + [shift(own, "tile_0", -r) for r in (1, 2, 3)]
    return column + [shift(block, "tile_1", 1) for block in column]


def from_all(rows):
    return lax.all_to_all(rows, TILE + SLAB, 0, 0, tiled=True)


def shards(volume, measured, weights, footprints, foot_pixel, foot_strip):
    owner = foot_strip // 32
    core = (owner & 1) ^ lax.axis_index("tile_1")
    ahead = ((owner >> 1) - lax.axis_index("tile_0")) & 3
    meta = (core * 4 + ahead) * 8 + (foot_strip // 4) % 8 + (foot_strip % 4) * 64 + foot_pixel * 256

    half, field = (4,) + RAY, (32, 32, 128)
    scratch = [pltpu.VMEM(field, BF16), pltpu.VMEM(field, BF16), pltpu.VMEM((64, 32, 128), F32)]
    mine, theirs = call(first_kernel, [half, half], [meta, footprints, volume], scratch, 1)
    parts = summed_by_owner(mine, theirs)
    residual, sent = call(start_kernel, [RAY, RAY], [*parts, measured, weights])

    mine, theirs, grad, norm0 = call(
        second_kernel, [half, half, field, (1, 8, 128)], [meta, footprints, *to_everyone(sent)], scratch, 1
    )
    parts = summed_by_owner(mine, theirs)
    p0, sent, curve0 = call(middle_kernel, [RAY, RAY, (1, 8, 128)], [*parts, weights])

    edge = (3, 32, 8, 128)
    mine, theirs, turned, sums, first, last = call(
        third_kernel,
        [half, half, field, (2, 8, 128), edge, edge],
        [meta, footprints, *to_everyone(sent), volume, grad],
        scratch,
        1,
    )
    slabs = lax.axis_size(SLAB)
    place_in = lax.axis_index(SLAB)
    ends = jnp.stack([place_in == 0, place_in == slabs - 1]).astype(jnp.int32)
    up = [(i, i + 1) for i in range(slabs - 1)]
    down = [(j, i) for i, j in up]
    last = lax.ppermute(last, SLAB, up)
    first = lax.ppermute(first, SLAB, down)
    parts = summed_by_owner(mine, theirs)
    everyone = slabs * lax.axis_size(TILE)
    q0, rows = call(
        end_kernel, [RAY, (everyone, 128)], [*parts, weights, p0, norm0, curve0, sums]
    )
    rows = from_all(rows)
    alphas, again = pl.pallas_call(
        judge_kernel,
        out_shape=[jax.ShapeDtypeStruct((2,), F32), jax.ShapeDtypeStruct((1,), jnp.int32)],
        in_specs=[VM],
        out_specs=[SM, SM],
        compiler_params=pltpu.CompilerParams(vmem_limit_bytes=8 << 20),
    )(rows)

    def summed_again(alphas):
        rows = call(
            again_kernel, [(everyone, 128)], [alphas, weights, p0, q0, grad, turned], (), 1
        )[0]
        return pl.pallas_call(
            ratio_kernel,
            out_shape=jax.ShapeDtypeStruct((2,), F32),
            in_specs=[SM, VM],
            out_specs=SM,
            compiler_params=pltpu.CompilerParams(vmem_limit_bytes=8 << 20),
        )(alphas, from_all(rows))

    alphas = lax.cond(again[0] == 1, summed_again, lambda known: known, alphas)
    return call(
        smooth_kernel,
        [volume.shape, measured.shape],
        [ends, alphas, volume, grad, turned, first, last, residual, p0, q0],
        (),
        2,
    )


def solution(mesh):
    finer = Mesh(mesh.devices.reshape(4, 2, 4, 4), ("tile_0", "tile_1", "slab_0", "slab_1"))
    return jax.shard_map(
        lambda *args: tuple(shards(*args)),
        mesh=finer,
        in_specs=(
            P(SLAB, TILE),
            P(SLAB, TILE),
            P(SLAB, TILE),
            P(TILE, None, None),
            P(TILE),
            P(TILE),
        ),
        out_specs=(P(SLAB, TILE), P(SLAB, TILE)),
        check_vma=False,
    )
```

```python
import jax
import jax.numpy as jnp
from jax import lax
from jax.experimental import pallas as pl
from jax.experimental.pallas import tpu as pltpu
from jax.sharding import Mesh
from jax.sharding import PartitionSpec as P

PASSES = 3
TILE = ("tile_0", "tile_1")
SLAB = ("slab_0", "slab_1")
GROUP = 4
UNROLL = 16
CHUNKS = 4

huber_width = 0.5
smooth_rate = 0.2


VM = pl.BlockSpec(memory_space=pltpu.VMEM)
SM = pl.BlockSpec(memory_space=pltpu.SMEM)
AN = pl.BlockSpec(memory_space=pltpu.HBM)
F32 = jnp.float32
BF16 = jnp.bfloat16


def call(kernel, outs, ins, scratch=(), smem=0, flops=1000000, limit=24, any_at=()):
    specs = [AN if n in any_at else SM if n < smem else VM for n in range(len(ins))]
    return pl.pallas_call(
        kernel,
        out_shape=[s if hasattr(s, "dtype") else jax.ShapeDtypeStruct(s, F32) for s in outs],
        in_specs=specs,
        out_specs=[VM] * len(outs),
        scratch_shapes=list(scratch),
        compiler_params=pltpu.CompilerParams(vmem_limit_bytes=limit << 20),
        cost_estimate=pl.CostEstimate(flops=flops, bytes_accessed=1 << 20, transcendentals=0),
    )(*ins)


def halves(value):
    high = value.astype(BF16)
    return high, (value - high.astype(F32)).astype(BF16)


def lane_groups(shape):
    return lax.broadcasted_iota(jnp.int32, shape, 1) // 32


def place(spots, b):
    pixels, strips, me = spots
    strip = strips[b]
    owner = strip >> 5
    slot = (((owner & 1) ^ me[1]) << 2) | (((owner >> 1) - me[0]) & 3)
    return (slot << 3) | ((strip >> 2) & 7), strip & 3, pixels[b]


def stacked(pair):
    high = pair[:, :128]
    return jnp.concatenate([pair, jnp.concatenate([high, jnp.zeros_like(high)], axis=1)], axis=0)


def forward_step(spots, g, pair, high, low, rays, groups):
    where = [place(spots, GROUP * g + i) for i in range(GROUP)]
    left = jnp.concatenate([jnp.concatenate([high[w[2]], low[w[2]]], axis=1) for w in where], axis=0)
    both = lax.dot_general(left, stacked(pair), (((1,), (0,)), ((), ())), preferred_element_type=F32)
    product = both[:, :128] + both[:, 128:]
    for i, (entry, spot, _) in enumerate(where):
        own = jnp.where(groups == i, product[32 * i : 32 * i + 32], 0.0)
        rays[entry] += pltpu.roll(own, ((spot - i) & 3) * 32, 1)


def forward_loop(spots, turned, high, low, rays):
    rays[...] = jnp.zeros_like(rays)
    groups = lane_groups((32, 128))

    def step(g, carry):
        forward_step(spots, g, turned[g], high, low, rays, groups)
        return carry

    lax.fori_loop(0, turned.shape[0], step, 0, unroll=UNROLL)


def back_loop(spots, plain, rays, field):
    field[...] = jnp.zeros_like(field)
    groups = lane_groups((32, 128))

    def step(g, carry):
        where = [place(spots, GROUP * g + i) for i in range(GROUP)]
        rows = []
        for i, (entry, spot, _) in enumerate(where):
            turned = pltpu.roll(rays[entry], ((i - spot) & 3) * 32, 1)
            own = jnp.where(groups == i, turned, 0.0)
            rows.append(jnp.concatenate(halves(own), axis=1))
        left = jnp.concatenate(rows, axis=0)
        both = lax.dot_general(
            left, stacked(plain[g]), (((1,), (0,)), ((), ())), preferred_element_type=F32
        )
        product = both[:, :128] + both[:, 128:]
        for i, (_, _, pixel) in enumerate(where):
            field[pixel] += product[32 * i : 32 * i + 32]
        return carry

    lax.fori_loop(0, plain.shape[0], step, 0, unroll=UNROLL)


def hand_out(rays, parts):
    for slot, part in enumerate(parts):
        part[...] = rays[8 * slot : 8 * slot + 8]


def first_kernel(pixels_hbm, strips_hbm, me, foot_hbm, volume_hbm, *refs):
    parts, (plain, turned, foot, volume, high, low, rays, pixels, strips, sem, foot_sem) = refs[:8], refs[8:]
    spots = (pixels, strips, me)
    per = foot.shape[0] // CHUNKS

    def chunk(t):
        some = pl.ds(t * per, per)
        return pltpu.make_async_copy(foot_hbm.at[some], foot.at[some], foot_sem.at[t])

    field = pltpu.make_async_copy(volume_hbm, volume, sem.at[0])
    field.start()
    indices = [
        pltpu.make_async_copy(pixels_hbm, pixels, sem.at[1]),
        pltpu.make_async_copy(strips_hbm, strips, sem.at[2]),
    ]
    for copy in indices:
        copy.start()
    for t in range(CHUNKS):
        chunk(t).start()
    rays[...] = jnp.zeros_like(rays)
    groups = lane_groups((32, 128))
    for copy in (*indices, field):
        copy.wait()
    for p in range(high.shape[0]):
        high[p], low[p] = halves(volume[:, 128 * p : 128 * p + 128])

    def trip(t, carry):
        chunk(t).wait()
        for u in range(per // GROUP):
            g = t * (per // GROUP) + u
            block = foot[pl.ds(GROUP * g, GROUP)].reshape(GROUP * 32, 128)
            plain[g] = jnp.concatenate(halves(block), axis=1)
            pair = jnp.concatenate(halves(block.T), axis=1)
            turned[g] = pair
            forward_step(spots, g, pair, high, low, rays, groups)
        return carry

    lax.fori_loop(0, CHUNKS, trip, 0)
    hand_out(rays, parts)


def folded(value):
    return jnp.sum(value.reshape(-1, 8, 128), axis=0)


def there_and_back(spots, plain, turned, pieces, parts, field, high, low, rays):
    for slot, piece in enumerate(pieces):
        rays[8 * slot : 8 * slot + 8] = piece[...]
    back_loop(spots, plain, rays, field)
    for p in range(high.shape[0]):
        high[p], low[p] = halves(field[p])
    forward_loop(spots, turned, high, low, rays)
    hand_out(rays, parts)


def second_kernel(pixels, strips, me, plain, turned, *refs):
    pieces, parts, (field, sums, high, low, rays) = refs[:8], refs[8:16], refs[16:]
    there_and_back((pixels, strips, me), plain, turned, pieces, parts, field, high, low, rays)
    sums[0] = folded(field[...] * field[...])


def third_kernel(pixels, strips, me, plain, turned, *refs):
    pieces, grad, parts = refs[:8], refs[8], refs[9:17]
    field, sums, first, last, high, low, rays = refs[17:]
    there_and_back((pixels, strips, me), plain, turned, pieces, parts, field, high, low, rays)
    sums[0] = folded(grad[...] * field[...])
    sums[1] = folded(field[...] * field[...])
    row = lax.broadcasted_iota(jnp.int32, (8, 128), 0)
    for p in range(field.shape[0]):
        first[p] = jnp.where(row < 3, grad[p, 0:8], pltpu.roll(field[p, 0:8], 3, 0))
        last[p] = jnp.where(row > 4, grad[p, 24:32], pltpu.roll(field[p, 24:32], 5, 0))


def add_kernel(one, other, out):
    out[...] = one[...] + other[...]


def tile_cols(ref):
    return jnp.stack([ref[:, 128 * t : 128 * t + 128] for t in range(ref.shape[1] // 128)])


def start_kernel(own, got, a, b, c, measured, weights, residual, sent):
    value = own[...] + got[...] + a[...] + b[...] + c[...] - tile_cols(measured)
    residual[...] = value
    sent[...] = tile_cols(weights) * value


def middle_kernel(own, got, a, b, c, weights, projected, sent, sums):
    value = own[...] + got[...] + a[...] + b[...] + c[...]
    weighted = tile_cols(weights) * value
    projected[...] = value
    sent[...] = weighted
    sums[0] = folded(weighted * value)


def in_lanes(sums, shape):
    lane = lax.broadcasted_iota(jnp.int32, shape, 1)
    value = jnp.zeros(shape, F32)
    for n, part in enumerate(sums):
        value = jnp.where(lane == n, jnp.sum(part, keepdims=True), value)
    return value


def end_kernel(own, got, a, b, c, weights, before, norm0, curve0, turned, projected, sums):
    value = own[...] + got[...] + a[...] + b[...] + c[...]
    weighted = tile_cols(weights) * value
    projected[...] = value
    cross = folded(weighted * before[...])
    sums[...] = in_lanes([norm0[0], curve0[0], turned[0], turned[1], cross, folded(weighted * value)], sums.shape)


def totals(rows, count):
    value = jnp.sum(rows[...], axis=0, keepdims=True)
    return [jnp.sum(value[:, n : n + 1]) for n in range(count)]


def judge_kernel(rows, alphas, again):
    norm0, curve0, cross_g, square_g, cross_p, square_p = totals(rows, 6)
    alpha = norm0 / curve0
    norm1 = norm0 - 2.0 * alpha * cross_g + alpha * alpha * square_g
    curve1 = curve0 - 2.0 * alpha * cross_p + alpha * alpha * square_p
    sound = (norm1 > 0.01 * norm0) & (curve1 > 0.01 * curve0)
    for square in (square_g, square_p):
        sound = sound & (square > 1e-25) & (square < 1e37)
    alphas[0] = alpha
    alphas[1] = norm1 / curve1
    again[0] = jnp.where(sound, 0, 1)


def again_kernel(alphas, weights, p0, q0, grad, turned, sums):
    value = p0[...] - alphas[0] * q0[...]
    step = grad[...] - alphas[0] * turned[...]
    sums[...] = in_lanes([folded(step * step), folded(tile_cols(weights) * value * value)], sums.shape)


def spread_kernel(own, got, rows):
    rows[...] = jnp.broadcast_to(own[0:1] + got[0:1], rows.shape)


def ratio_kernel(alphas, rows, out):
    norm1, curve1 = totals(rows, 2)
    out[0] = alphas[0]
    out[1] = norm1 / curve1


def smooth_kernel(ends, alphas, volume, grad, turned, first0, last0, first, last, residual, p0, q0, smoothed, left_over):
    alpha0, alpha1 = alphas[0], alphas[1]
    rest = residual[...] - alpha0 * p0[...] - alpha1 * (p0[...] - alpha0 * q0[...])
    for t in range(rest.shape[0]):
        left_over[:, 128 * t : 128 * t + 128] = rest[t]

    def stepped(x, g, h):
        return x - alpha0 * g - alpha1 * (g - alpha0 * h)

    row = lax.broadcasted_iota(jnp.int32, (48, 128), 0)
    open_link = ~(((row == 7) & (ends[0] == 1)) | ((row == 39) & (ends[1] == 1)))
    link = jnp.where(open_link, F32(1.0), F32(0.0))
    for p in range(grad.shape[0]):
        cols = slice(128 * p, 128 * p + 128)
        ext = jnp.concatenate(
            [
                stepped(last0[:, cols], last[p], pltpu.roll(last[p], 3, 0)),
                stepped(volume[:, cols], grad[p], turned[p]),
                stepped(first0[:, cols], first[p], pltpu.roll(first[p], 5, 0)),
            ],
            axis=0,
        )
        for _ in range(PASSES):
            clipped = jnp.clip(pltpu.roll(ext, 47, 0) - ext, -huber_width, huber_width) * link
            ext = ext + smooth_rate * (clipped - pltpu.roll(clipped, 1, 0))
        smoothed[:, cols] = ext[8:40]


def shift(value, axis, by):
    n = lax.axis_size(axis)
    return lax.ppermute(value, axis, [(i, (i + by) % n) for i in range(n)])


RAY = (8, 32, 128)


def summed_by_owner(parts):
    own, theirs = parts[:4], parts[4:8]
    got, moved = {}, {}
    for r in (2, 1, 3, 0):
        got[r] = shift(theirs[r], "tile_1", 1)
    for r in (2, 1, 3):
        part = call(add_kernel, [RAY], [own[r], got[r]])[0]
        moved[r] = shift(part, "tile_0", r)
    return own[0], got[0], moved[1], moved[2], moved[3]


def to_everyone(own):
    column = [own] + [shift(own, "tile_0", -r) for r in (1, 2, 3)]
    return column + [shift(block, "tile_1", 1) for block in column]


def over_all(sums):
    got = shift(sums, "tile_1", 1)
    axes = ("tile_0",) + SLAB
    rows = call(spread_kernel, [(lax.axis_size(axes), 128)], [sums, got])[0]
    return lax.all_to_all(rows, axes, 0, 0, tiled=True)


def shards(volume, measured, weights, footprints, foot_pixel, foot_strip):
    me = jnp.stack([lax.axis_index("tile_0"), lax.axis_index("tile_1")])
    spots = [foot_pixel, foot_strip, me]
    slabs = lax.axis_size(SLAB)
    place_in = lax.axis_index(SLAB)
    ends = jnp.stack([place_in == 0, place_in == slabs - 1]).astype(jnp.int32)
    up = [(i, i + 1) for i in range(slabs - 1)]
    down = [(j, i) for i, j in up]

    field, tile = (32, 32, 128), (1, 8, 128)
    scratch = [pltpu.VMEM(field, BF16), pltpu.VMEM(field, BF16), pltpu.VMEM((64, 32, 128), F32)]
    streams = [
        pltpu.VMEM(footprints.shape, F32),
        pltpu.VMEM(volume.shape, F32),
        *scratch,
        pltpu.SMEM(foot_pixel.shape, jnp.int32),
        pltpu.SMEM(foot_strip.shape, jnp.int32),
        pltpu.SemaphoreType.DMA((3,)),
        pltpu.SemaphoreType.DMA((CHUNKS,)),
    ]
    split = jax.ShapeDtypeStruct((64, 128, 256), BF16)
    *parts, plain, turned = call(
        first_kernel,
        [RAY] * 8 + [split, split],
        [*spots, footprints, volume],
        streams,
        3,
        any_at=(0, 1, 3, 4),
        limit=32,
    )
    last0 = lax.ppermute(volume[24:32], SLAB, up)
    first0 = lax.ppermute(volume[0:8], SLAB, down)
    parts = summed_by_owner(parts)
    residual, sent = call(start_kernel, [RAY, RAY], [*parts, measured, weights])

    *parts, grad, norm0 = call(
        second_kernel, [RAY] * 8 + [field, tile], [*spots, plain, turned, *to_everyone(sent)], scratch, 3
    )
    parts = summed_by_owner(parts)
    p0, sent, curve0 = call(middle_kernel, [RAY, RAY, tile], [*parts, weights])

    edge = (32, 8, 128)
    *parts, back, crossed, first, last = call(
        third_kernel,
        [RAY] * 8 + [field, (2, 8, 128), edge, edge],
        [*spots, plain, turned, *to_everyone(sent), grad],
        scratch,
        3,
    )
    last = lax.ppermute(last, SLAB, up)
    first = lax.ppermute(first, SLAB, down)
    parts = summed_by_owner(parts)
    q0, sums = call(end_kernel, [RAY, (8, 128)], [*parts, weights, p0, norm0, curve0, crossed])
    rows = over_all(sums)
    alphas, again = pl.pallas_call(
        judge_kernel,
        out_shape=[jax.ShapeDtypeStruct((2,), F32), jax.ShapeDtypeStruct((1,), jnp.int32)],
        in_specs=[VM],
        out_specs=[SM, SM],
        compiler_params=pltpu.CompilerParams(vmem_limit_bytes=8 << 20),
    )(rows)

    def summed_again(alphas):
        sums = call(again_kernel, [(8, 128)], [alphas, weights, p0, q0, grad, back], (), 1)[0]
        return pl.pallas_call(
            ratio_kernel,
            out_shape=jax.ShapeDtypeStruct((2,), F32),
            in_specs=[SM, VM],
            out_specs=SM,
            compiler_params=pltpu.CompilerParams(vmem_limit_bytes=8 << 20),
        )(alphas, over_all(sums))

    alphas = lax.cond(again[0] == 1, summed_again, lambda known: known, alphas)
    return call(
        smooth_kernel,
        [volume.shape, measured.shape],
        [ends, alphas, volume, grad, back, first0, last0, first, last, residual, p0, q0],
        (),
        2,
    )


def solution(mesh):
    finer = Mesh(mesh.devices.reshape(4, 2, 4, 4), ("tile_0", "tile_1", "slab_0", "slab_1"))
    return jax.shard_map(
        lambda *args: tuple(shards(*args)),
        mesh=finer,
        in_specs=(
            P(SLAB, TILE),
            P(SLAB, TILE),
            P(SLAB, TILE),
            P(TILE, None, None),
            P(TILE),
            P(TILE),
        ),
        out_specs=(P(SLAB, TILE), P(SLAB, TILE)),
        check_vma=False,
    )
```

```python
import jax
import jax.numpy as jnp
from jax import lax
from jax.experimental import pallas as pl
from jax.experimental.pallas import tpu as pltpu
from jax.sharding import Mesh
from jax.sharding import PartitionSpec as P

PASSES = 3
TILE = ("tile_0", "tile_1")
SLAB = ("slab_0", "slab_1")
GROUP = 4
UNROLL = 16
CHUNKS = 4

huber_width = 0.5
smooth_rate = 0.2


VM = pl.BlockSpec(memory_space=pltpu.VMEM)
SM = pl.BlockSpec(memory_space=pltpu.SMEM)
AN = pl.BlockSpec(memory_space=pltpu.HBM)
F32 = jnp.float32
BF16 = jnp.bfloat16


def call(kernel, outs, ins, scratch=(), smem=0, flops=1000000, limit=24, any_at=()):
    specs = [AN if n in any_at else SM if n < smem else VM for n in range(len(ins))]
    return pl.pallas_call(
        kernel,
        out_shape=[s if hasattr(s, "dtype") else jax.ShapeDtypeStruct(s, F32) for s in outs],
        in_specs=specs,
        out_specs=[VM] * len(outs),
        scratch_shapes=list(scratch),
        compiler_params=pltpu.CompilerParams(vmem_limit_bytes=limit << 20),
        cost_estimate=pl.CostEstimate(flops=flops, bytes_accessed=1 << 20, transcendentals=0),
    )(*ins)


def halves(value):
    high = value.astype(BF16)
    return high, (value - high.astype(F32)).astype(BF16)


def lane_groups(shape):
    return lax.broadcasted_iota(jnp.int32, shape, 1) // 32


def place(spots, b):
    pixels, strips, me = spots
    strip = strips[b]
    owner = strip >> 5
    slot = (((owner & 1) ^ me[1]) << 2) | (((owner >> 1) - me[0]) & 3)
    return (slot << 3) | ((strip >> 2) & 7), strip & 3, pixels[b]


def stacked(pair):
    high = pair[:, :128]
    return jnp.concatenate([pair, jnp.concatenate([high, jnp.zeros_like(high)], axis=1)], axis=0)


def forward_step(spots, g, pair, high, low, rays, groups):
    where = [place(spots, GROUP * g + i) for i in range(GROUP)]
    left = jnp.concatenate([jnp.concatenate([high[w[2]], low[w[2]]], axis=1) for w in where], axis=0)
    both = lax.dot_general(left, stacked(pair), (((1,), (0,)), ((), ())), preferred_element_type=F32)
    product = both[:, :128] + both[:, 128:]
    for i, (entry, spot, _) in enumerate(where):
        own = jnp.where(groups == i, product[32 * i : 32 * i + 32], 0.0)
        rays[entry] += pltpu.roll(own, ((spot - i) & 3) * 32, 1)


def forward_loop(spots, turned, high, low, rays):
    rays[...] = jnp.zeros_like(rays)
    groups = lane_groups((32, 128))

    def step(g, carry):
        forward_step(spots, g, turned[g], high, low, rays, groups)
        return carry

    lax.fori_loop(0, turned.shape[0], step, 0, unroll=UNROLL)


def back_loop(spots, plain, rays, field):
    field[...] = jnp.zeros_like(field)
    groups = lane_groups((32, 128))

    def step(g, carry):
        where = [place(spots, GROUP * g + i) for i in range(GROUP)]
        rows = []
        for i, (entry, spot, _) in enumerate(where):
            turned = pltpu.roll(rays[entry], ((i - spot) & 3) * 32, 1)
            own = jnp.where(groups == i, turned, 0.0)
            rows.append(jnp.concatenate(halves(own), axis=1))
        left = jnp.concatenate(rows, axis=0)
        both = lax.dot_general(
            left, stacked(plain[g]), (((1,), (0,)), ((), ())), preferred_element_type=F32
        )
        product = both[:, :128] + both[:, 128:]
        for i, (_, _, pixel) in enumerate(where):
            field[pixel] += product[32 * i : 32 * i + 32]
        return carry

    lax.fori_loop(0, plain.shape[0], step, 0, unroll=UNROLL)


def hand_out(rays, mine, theirs):
    mine[...] = rays[:32].reshape(mine.shape)
    theirs[...] = rays[32:].reshape(theirs.shape)


def first_kernel(pixels_hbm, strips_hbm, me, foot_hbm, volume_hbm, *refs):
    mine, theirs, first, last, plain, turned, foot, volume, high, low, rays, pixels, strips, sem, foot_sem = refs
    spots = (pixels, strips, me)
    per = foot.shape[0] // CHUNKS

    def chunk(t):
        some = pl.ds(t * per, per)
        return pltpu.make_async_copy(foot_hbm.at[some], foot.at[some], foot_sem.at[t])

    field = pltpu.make_async_copy(volume_hbm, volume, sem.at[0])
    field.start()
    indices = [
        pltpu.make_async_copy(pixels_hbm, pixels, sem.at[1]),
        pltpu.make_async_copy(strips_hbm, strips, sem.at[2]),
    ]
    for copy in indices:
        copy.start()
    for t in range(CHUNKS):
        chunk(t).start()
    rays[...] = jnp.zeros_like(rays)
    groups = lane_groups((32, 128))
    for copy in (*indices, field):
        copy.wait()
    for p in range(high.shape[0]):
        cols = slice(128 * p, 128 * p + 128)
        high[p], low[p] = halves(volume[:, cols])
        first[p], last[p] = volume[0:8, cols], volume[24:32, cols]

    def trip(t, carry):
        chunk(t).wait()
        for u in range(per // GROUP):
            g = t * (per // GROUP) + u
            block = foot[pl.ds(GROUP * g, GROUP)].reshape(GROUP * 32, 128)
            plain[g] = jnp.concatenate(halves(block), axis=1)
            pair = jnp.concatenate(halves(block.T), axis=1)
            turned[g] = pair
            forward_step(spots, g, pair, high, low, rays, groups)
        return carry

    lax.fori_loop(0, CHUNKS, trip, 0)
    hand_out(rays, mine, theirs)


def folded(value):
    return jnp.sum(value.reshape(-1, 8, 128), axis=0)


def there_and_back(spots, plain, turned, pieces, mine, theirs, field, high, low, rays):
    for slot, piece in enumerate(pieces):
        rays[8 * slot : 8 * slot + 8] = piece[...]
    back_loop(spots, plain, rays, field)
    for p in range(high.shape[0]):
        high[p], low[p] = halves(field[p])
    forward_loop(spots, turned, high, low, rays)
    hand_out(rays, mine, theirs)


def second_kernel(pixels, strips, me, plain, turned, *refs):
    pieces, (mine, theirs, field, sums, high, low, rays) = refs[:8], refs[8:]
    there_and_back((pixels, strips, me), plain, turned, pieces, mine, theirs, field, high, low, rays)
    sums[0] = folded(field[...] * field[...])


def third_kernel(pixels, strips, me, plain, turned, *refs):
    pieces, grad = refs[:8], refs[8]
    mine, theirs, field, sums, first, last, high, low, rays = refs[9:]
    there_and_back((pixels, strips, me), plain, turned, pieces, mine, theirs, field, high, low, rays)
    sums[0] = folded(grad[...] * field[...])
    sums[1] = folded(field[...] * field[...])
    row = lax.broadcasted_iota(jnp.int32, (8, 128), 0)
    for p in range(field.shape[0]):
        first[p] = jnp.where(row < 3, grad[p, 0:8], pltpu.roll(field[p, 0:8], 3, 0))
        last[p] = jnp.where(row > 4, grad[p, 24:32], pltpu.roll(field[p, 24:32], 5, 0))


def add_kernel(mine, got, kept, s1, s2, s3):
    for r, out in enumerate((kept, s1, s2, s3)):
        out[...] = mine[r] + got[r]


def tile_cols(ref):
    return jnp.stack([ref[:, 128 * t : 128 * t + 128] for t in range(ref.shape[1] // 128)])


def start_kernel(kept, a, b, c, measured, weights, residual, sent):
    value = kept[...] + a[...] + b[...] + c[...] - tile_cols(measured)
    residual[...] = value
    sent[...] = tile_cols(weights) * value


def middle_kernel(kept, a, b, c, weights, projected, sent, sums):
    value = kept[...] + a[...] + b[...] + c[...]
    weighted = tile_cols(weights) * value
    projected[...] = value
    sent[...] = weighted
    sums[0] = folded(weighted * value)


def in_lanes(sums, shape):
    lane = lax.broadcasted_iota(jnp.int32, shape, 1)
    value = jnp.zeros(shape, F32)
    for n, part in enumerate(sums):
        value = jnp.where(lane == n, jnp.sum(part, keepdims=True), value)
    return value


def end_kernel(kept, a, b, c, weights, before, norm0, curve0, turned, projected, rows):
    value = kept[...] + a[...] + b[...] + c[...]
    weighted = tile_cols(weights) * value
    projected[...] = value
    cross = folded(weighted * before[...])
    rows[...] = in_lanes([norm0[0], curve0[0], turned[0], turned[1], cross, folded(weighted * value)], rows.shape)


def totals(rows, count):
    value = jnp.sum(rows[...], axis=0, keepdims=True)
    return [jnp.sum(value[:, n : n + 1]) for n in range(count)]


def judge_kernel(rows, alphas, again):
    norm0, curve0, cross_g, square_g, cross_p, square_p = totals(rows, 6)
    alpha = norm0 / curve0
    norm1 = norm0 - 2.0 * alpha * cross_g + alpha * alpha * square_g
    curve1 = curve0 - 2.0 * alpha * cross_p + alpha * alpha * square_p
    sound = (norm1 > 0.01 * norm0) & (curve1 > 0.01 * curve0)
    for square in (square_g, square_p):
        sound = sound & (square > 1e-25) & (square < 1e37)
    alphas[0] = alpha
    alphas[1] = norm1 / curve1
    again[0] = jnp.where(sound, 0, 1)


def again_kernel(alphas, weights, p0, q0, grad, turned, rows):
    value = p0[...] - alphas[0] * q0[...]
    step = grad[...] - alphas[0] * turned[...]
    rows[...] = in_lanes([folded(step * step), folded(tile_cols(weights) * value * value)], rows.shape)


def ratio_kernel(alphas, rows, out):
    norm1, curve1 = totals(rows, 2)
    out[0] = alphas[0]
    out[1] = norm1 / curve1


def smooth_kernel(ends, alphas, volume, grad, turned, first0, last0, first, last, residual, p0, q0, smoothed, left_over):
    alpha0, alpha1 = alphas[0], alphas[1]
    rest = residual[...] - alpha0 * p0[...] - alpha1 * (p0[...] - alpha0 * q0[...])
    for t in range(rest.shape[0]):
        left_over[:, 128 * t : 128 * t + 128] = rest[t]

    def stepped(x, g, h):
        return x - alpha0 * g - alpha1 * (g - alpha0 * h)

    row = lax.broadcasted_iota(jnp.int32, (48, 128), 0)
    open_link = ~(((row == 7) & (ends[0] == 1)) | ((row == 39) & (ends[1] == 1)))
    link = jnp.where(open_link, F32(1.0), F32(0.0))
    for p in range(grad.shape[0]):
        cols = slice(128 * p, 128 * p + 128)
        ext = jnp.concatenate(
            [
                stepped(last0[p], last[p], pltpu.roll(last[p], 3, 0)),
                stepped(volume[:, cols], grad[p], turned[p]),
                stepped(first0[p], first[p], pltpu.roll(first[p], 5, 0)),
            ],
            axis=0,
        )
        for _ in range(PASSES):
            clipped = jnp.clip(pltpu.roll(ext, 47, 0) - ext, -huber_width, huber_width) * link
            ext = ext + smooth_rate * (clipped - pltpu.roll(clipped, 1, 0))
        smoothed[:, cols] = ext[8:40]


def shift(value, axis, by):
    n = lax.axis_size(axis)
    return lax.ppermute(value, axis, [(i, (i + by) % n) for i in range(n)])


RAY = (8, 32, 128)


def summed_by_owner(mine, theirs):
    got = shift(theirs, "tile_1", 1)
    kept, s1, s2, s3 = call(add_kernel, [RAY] * 4, [mine, got])
    return kept, shift(s1, "tile_0", 1), shift(s2, "tile_0", 2), shift(s3, "tile_0", 3)


def to_everyone(own):
    column = [own] + [shift(own, "tile_0", -r) for r in (1, 2, 3)]
    return column + [shift(block, "tile_1", 1) for block in column]


def over_all(rows):
    return lax.all_to_all(rows, TILE + SLAB, 0, 0, tiled=True)


def shards(volume, measured, weights, footprints, foot_pixel, foot_strip):
    me = jnp.stack([lax.axis_index("tile_0"), lax.axis_index("tile_1")])
    spots = [foot_pixel, foot_strip, me]
    slabs = lax.axis_size(SLAB)
    place_in = lax.axis_index(SLAB)
    ends = jnp.stack([place_in == 0, place_in == slabs - 1]).astype(jnp.int32)
    up = [(i, i + 1) for i in range(slabs - 1)]
    down = [(j, i) for i, j in up]

    field, tile = (32, 32, 128), (1, 8, 128)
    scratch = [pltpu.VMEM(field, BF16), pltpu.VMEM(field, BF16), pltpu.VMEM((64, 32, 128), F32)]
    in_place = [pltpu.with_memory_space_constraint(x, pltpu.HBM) for x in (foot_pixel, foot_strip, footprints, volume)]
    streams = [
        pltpu.VMEM(footprints.shape, F32),
        pltpu.VMEM(volume.shape, F32),
        *scratch,
        pltpu.SMEM(foot_pixel.shape, jnp.int32),
        pltpu.SMEM(foot_strip.shape, jnp.int32),
        pltpu.SemaphoreType.DMA((3,)),
        pltpu.SemaphoreType.DMA((CHUNKS,)),
    ]
    split = jax.ShapeDtypeStruct((64, 128, 256), BF16)
    half, edge = (4,) + RAY, (32, 8, 128)
    mine, theirs, first0, last0, plain, turned = call(
        first_kernel,
        [half, half, edge, edge, split, split],
        [*in_place[:2], me, *in_place[2:]],
        streams,
        3,
        any_at=(0, 1, 3, 4),
        limit=32,
    )
    parts = summed_by_owner(mine, theirs)
    with jax.named_scope("edge"):
        first0, last0 = lax.ppermute(first0, SLAB, down), lax.ppermute(last0, SLAB, up)
    residual, sent = call(start_kernel, [RAY, RAY], [*parts, measured, weights])
    pieces, first0, last0 = lax.optimization_barrier((to_everyone(sent), first0, last0))

    mine, theirs, grad, norm0 = call(
        second_kernel, [half, half, field, tile], [*spots, plain, turned, *pieces], scratch, 3
    )
    parts = summed_by_owner(mine, theirs)
    p0, sent, curve0 = call(middle_kernel, [RAY, RAY, tile], [*parts, weights])

    mine, theirs, back, crossed, first, last = call(
        third_kernel,
        [half, half, field, (2, 8, 128), edge, edge],
        [*spots, plain, turned, *to_everyone(sent), grad],
        scratch,
        3,
    )
    with jax.named_scope("edge"):
        first, last = lax.ppermute(first, SLAB, down), lax.ppermute(last, SLAB, up)
    parts = summed_by_owner(mine, theirs)
    everyone = slabs * lax.axis_size(TILE)
    q0, rows = call(
        end_kernel, [RAY, (everyone, 128)], [*parts, weights, p0, norm0, curve0, crossed]
    )
    rows, first, last, ends = lax.optimization_barrier((rows, first, last, ends))
    rows = over_all(rows)
    alphas, again = pl.pallas_call(
        judge_kernel,
        out_shape=[jax.ShapeDtypeStruct((2,), F32), jax.ShapeDtypeStruct((1,), jnp.int32)],
        in_specs=[VM],
        out_specs=[SM, SM],
        compiler_params=pltpu.CompilerParams(vmem_limit_bytes=8 << 20),
    )(rows)

    def summed_again(alphas):
        rows = call(again_kernel, [(everyone, 128)], [alphas, weights, p0, q0, grad, back], (), 1)[0]
        return pl.pallas_call(
            ratio_kernel,
            out_shape=jax.ShapeDtypeStruct((2,), F32),
            in_specs=[SM, VM],
            out_specs=SM,
            compiler_params=pltpu.CompilerParams(vmem_limit_bytes=8 << 20),
        )(alphas, over_all(rows))

    alphas = lax.cond(again[0] == 1, summed_again, lambda known: known, alphas)
    return call(
        smooth_kernel,
        [volume.shape, measured.shape],
        [ends, alphas, volume, grad, back, first0, last0, first, last, residual, p0, q0],
        (),
        2,
    )


def solution(mesh):
    finer = Mesh(mesh.devices.reshape(4, 2, 4, 4), ("tile_0", "tile_1", "slab_0", "slab_1"))
    return jax.shard_map(
        lambda *args: tuple(shards(*args)),
        mesh=finer,
        in_specs=(
            P(SLAB, TILE),
            P(SLAB, TILE),
            P(SLAB, TILE),
            P(TILE, None, None),
            P(TILE),
            P(TILE),
        ),
        out_specs=(P(SLAB, TILE), P(SLAB, TILE)),
        check_vma=False,
    )
```

```python
import jax
import jax.numpy as jnp
from jax import lax
from jax.experimental import pallas as pl
from jax.experimental.pallas import tpu as pltpu
from jax.sharding import Mesh
from jax.sharding import PartitionSpec as P


PASSES = 3
TILE = ("tile_0", "tile_1")
SLAB = ("slab_0", "slab_1")
GROUP = 4
UNROLL = 32
CHUNKS = 4

huber_width = 0.5
smooth_rate = 0.2


VM = pl.BlockSpec(memory_space=pltpu.VMEM)
SM = pl.BlockSpec(memory_space=pltpu.SMEM)
AN = pl.BlockSpec(memory_space=pltpu.HBM)
F32 = jnp.float32
BF16 = jnp.bfloat16


def call(kernel, outs, ins, scratch=(), smem=0, flops=1000000, limit=24, any_at=()):
    specs = [AN if n in any_at else SM if n < smem else VM for n in range(len(ins))]
    return pl.pallas_call(
        kernel,
        out_shape=[s if hasattr(s, "dtype") else jax.ShapeDtypeStruct(s, F32) for s in outs],
        in_specs=specs,
        out_specs=[VM] * len(outs),
        scratch_shapes=list(scratch),
        compiler_params=pltpu.CompilerParams(vmem_limit_bytes=limit << 20),
        cost_estimate=pl.CostEstimate(flops=flops, bytes_accessed=1 << 20, transcendentals=0),
    )(*ins)


def halves(value):
    high = value.astype(BF16)
    return high, (value - high.astype(F32)).astype(BF16)


def lane_groups(shape):
    return lax.broadcasted_iota(jnp.int32, shape, 1) // 32


def place(spots, b):
    pixels, strips, me = spots
    strip = strips[b]
    owner = strip >> 5
    slot = (((owner & 1) ^ me[1]) << 2) | (((owner >> 1) - me[0]) & 3)
    return (slot << 3) | ((strip >> 2) & 7), strip & 3, pixels[b]


def stacked(pair):
    high = pair[:, :128]
    return jnp.concatenate([pair, jnp.concatenate([high, jnp.zeros_like(high)], axis=1)], axis=0)


def forward_step(spots, g, pair, high, low, rays, groups):
    where = [place(spots, GROUP * g + i) for i in range(GROUP)]
    left = jnp.concatenate([jnp.concatenate([high[w[2]], low[w[2]]], axis=1) for w in where], axis=0)
    both = lax.dot_general(left, stacked(pair), (((1,), (0,)), ((), ())), preferred_element_type=F32)
    product = both[:, :128] + both[:, 128:]
    for i, (entry, spot, _) in enumerate(where):
        own = jnp.where(groups == i, product[32 * i : 32 * i + 32], 0.0)
        rays[entry] += pltpu.roll(own, ((spot - i) & 3) * 32, 1)


def forward_loop(spots, turned, high, low, rays):
    rays[...] = jnp.zeros_like(rays)
    groups = lane_groups((32, 128))

    def step(g, carry):
        forward_step(spots, g, turned[g], high, low, rays, groups)
        return carry

    lax.fori_loop(0, turned.shape[0], step, 0, unroll=UNROLL)


def back_loop(spots, plain, rays, field):
    field[...] = jnp.zeros_like(field)
    groups = lane_groups((32, 128))

    def step(g, carry):
        where = [place(spots, GROUP * g + i) for i in range(GROUP)]
        rows = []
        for i, (entry, spot, _) in enumerate(where):
            turned = pltpu.roll(rays[entry], ((i - spot) & 3) * 32, 1)
            own = jnp.where(groups == i, turned, 0.0)
            rows.append(jnp.concatenate(halves(own), axis=1))
        left = jnp.concatenate(rows, axis=0)
        both = lax.dot_general(
            left, stacked(plain[g]), (((1,), (0,)), ((), ())), preferred_element_type=F32
        )
        product = both[:, :128] + both[:, 128:]
        for i, (_, _, pixel) in enumerate(where):
            field[pixel] += product[32 * i : 32 * i + 32]
        return carry

    lax.fori_loop(0, plain.shape[0], step, 0, unroll=UNROLL)


def hand_out(rays, mine, theirs):
    mine[...] = rays[:32].reshape(mine.shape)
    theirs[...] = rays[32:].reshape(theirs.shape)


def first_kernel(pixels_hbm, strips_hbm, me, foot_hbm, volume_hbm, *refs):
    mine, theirs, first, last, plain, turned, foot, volume, high, low, rays, pixels, strips, sem, foot_sem = refs
    spots = (pixels, strips, me)
    per = foot.shape[0] // CHUNKS

    def chunk(t):
        some = pl.ds(t * per, per)
        return pltpu.make_async_copy(foot_hbm.at[some], foot.at[some], foot_sem.at[t])

    field = pltpu.make_async_copy(volume_hbm, volume, sem.at[0])
    field.start()
    indices = [
        pltpu.make_async_copy(pixels_hbm, pixels, sem.at[1]),
        pltpu.make_async_copy(strips_hbm, strips, sem.at[2]),
    ]
    for copy in indices:
        copy.start()
    for t in range(CHUNKS):
        chunk(t).start()
    rays[...] = jnp.zeros_like(rays)
    groups = lane_groups((32, 128))
    for copy in (*indices, field):
        copy.wait()
    for p in range(high.shape[0]):
        cols = slice(128 * p, 128 * p + 128)
        high[p], low[p] = halves(volume[:, cols])
        first[p], last[p] = volume[0:8, cols], volume[24:32, cols]

    def trip(t, carry):
        chunk(t).wait()
        for u in range(per // GROUP):
            g = t * (per // GROUP) + u
            block = foot[pl.ds(GROUP * g, GROUP)].reshape(GROUP * 32, 128)
            plain[g] = jnp.concatenate(halves(block), axis=1)
            pair = jnp.concatenate(halves(block.T), axis=1)
            turned[g] = pair
            forward_step(spots, g, pair, high, low, rays, groups)
        return carry

    lax.fori_loop(0, CHUNKS, trip, 0)
    hand_out(rays, mine, theirs)


def folded(value):
    return jnp.sum(value.reshape(-1, 8, 128), axis=0)


def there_and_back(spots, plain, turned, pieces, mine, theirs, field, high, low, rays):
    for slot, piece in enumerate(pieces):
        rays[8 * slot : 8 * slot + 8] = piece[...]
    back_loop(spots, plain, rays, field)
    for p in range(high.shape[0]):
        high[p], low[p] = halves(field[p])
    forward_loop(spots, turned, high, low, rays)
    hand_out(rays, mine, theirs)


def second_kernel(pixels, strips, me, plain, turned, *refs):
    pieces, (mine, theirs, field, sums, high, low, rays) = refs[:8], refs[8:]
    there_and_back((pixels, strips, me), plain, turned, pieces, mine, theirs, field, high, low, rays)
    sums[0] = folded(field[...] * field[...])


def third_kernel(pixels, strips, me, plain, turned, *refs):
    pieces, grad = refs[:8], refs[8]
    mine, theirs, field, sums, first, last, high, low, rays = refs[9:]
    there_and_back((pixels, strips, me), plain, turned, pieces, mine, theirs, field, high, low, rays)
    sums[0] = folded(grad[...] * field[...])
    sums[1] = folded(field[...] * field[...])
    row = lax.broadcasted_iota(jnp.int32, (8, 128), 0)
    for p in range(field.shape[0]):
        first[p] = jnp.where(row < 3, grad[p, 0:8], pltpu.roll(field[p, 0:8], 3, 0))
        last[p] = jnp.where(row > 4, grad[p, 24:32], pltpu.roll(field[p, 24:32], 5, 0))


def add_kernel(mine, got, kept, s1, s2, s3):
    for r, out in enumerate((kept, s1, s2, s3)):
        out[...] = mine[r] + got[r]


def tile_cols(ref):
    return jnp.stack([ref[:, 128 * t : 128 * t + 128] for t in range(ref.shape[1] // 128)])


def start_kernel(kept, a, b, c, measured, weights, residual, sent):
    value = kept[...] + a[...] + b[...] + c[...] - tile_cols(measured)
    residual[...] = value
    sent[...] = tile_cols(weights) * value


def middle_kernel(kept, a, b, c, weights, projected, sent, sums):
    value = kept[...] + a[...] + b[...] + c[...]
    weighted = tile_cols(weights) * value
    projected[...] = value
    sent[...] = weighted
    sums[0] = folded(weighted * value)


def in_lanes(sums, shape):
    lane = lax.broadcasted_iota(jnp.int32, shape, 1)
    value = jnp.zeros(shape, F32)
    for n, part in enumerate(sums):
        value = jnp.where(lane == n, jnp.sum(part, keepdims=True), value)
    return value


def end_kernel(kept, a, b, c, weights, before, norm0, curve0, turned, projected, rows):
    value = kept[...] + a[...] + b[...] + c[...]
    weighted = tile_cols(weights) * value
    projected[...] = value
    cross = folded(weighted * before[...])
    rows[...] = in_lanes([norm0[0], curve0[0], turned[0], turned[1], cross, folded(weighted * value)], rows.shape)


def totals(rows, count):
    value = jnp.sum(rows[...], axis=0, keepdims=True)
    return [value[:, n : n + 1] for n in range(count)]


def scalar(value):
    return jnp.sum(value)


def judge_kernel(rows, alphas, again):
    norm0, curve0, cross_g, square_g, cross_p, square_p = totals(rows, 6)
    alpha = norm0 / curve0
    norm1 = norm0 - 2.0 * alpha * cross_g + alpha * alpha * square_g
    curve1 = curve0 - 2.0 * alpha * cross_p + alpha * alpha * square_p
    sound = (norm1 > 0.01 * norm0) & (curve1 > 0.01 * curve0)
    for square in (square_g, square_p):
        sound = sound & (square > 1e-25) & (square < 1e37)
    alphas[0] = scalar(alpha)
    alphas[1] = scalar(norm1 / curve1)
    again[0] = jnp.where(scalar(jnp.where(sound, F32(0.0), F32(1.0))) > 0.5, 1, 0)


def again_kernel(alphas, weights, p0, q0, grad, turned, rows):
    value = p0[...] - alphas[0] * q0[...]
    step = grad[...] - alphas[0] * turned[...]
    rows[...] = in_lanes([folded(step * step), folded(tile_cols(weights) * value * value)], rows.shape)


def ratio_kernel(alphas, rows, out):
    norm1, curve1 = totals(rows, 2)
    out[0] = alphas[0]
    out[1] = scalar(norm1 / curve1)


def smooth_kernel(ends, alphas, volume, grad, turned, first0, last0, first, last, residual, p0, q0, smoothed, left_over):
    alpha0, alpha1 = alphas[0], alphas[1]
    rest = residual[...] - alpha0 * p0[...] - alpha1 * (p0[...] - alpha0 * q0[...])
    for t in range(rest.shape[0]):
        left_over[:, 128 * t : 128 * t + 128] = rest[t]

    def stepped(x, g, h):
        return x - alpha0 * g - alpha1 * (g - alpha0 * h)

    row = lax.broadcasted_iota(jnp.int32, (48, 128), 0)
    open_link = ~(((row == 7) & (ends[0] == 1)) | ((row == 39) & (ends[1] == 1)))
    link = jnp.where(open_link, F32(1.0), F32(0.0))
    for p in range(grad.shape[0]):
        cols = slice(128 * p, 128 * p + 128)
        ext = jnp.concatenate(
            [
                stepped(last0[p], last[p], pltpu.roll(last[p], 3, 0)),
                stepped(volume[:, cols], grad[p], turned[p]),
                stepped(first0[p], first[p], pltpu.roll(first[p], 5, 0)),
            ],
            axis=0,
        )
        for _ in range(PASSES):
            clipped = jnp.clip(pltpu.roll(ext, 47, 0) - ext, -huber_width, huber_width) * link
            ext = ext + smooth_rate * (clipped - pltpu.roll(clipped, 1, 0))
        smoothed[:, cols] = ext[8:40]


def shift(value, axis, by):
    n = lax.axis_size(axis)
    return lax.ppermute(value, axis, [(i, (i + by) % n) for i in range(n)])


RAY = (8, 32, 128)


def summed_by_owner(mine, theirs):
    got = shift(theirs, "tile_1", 1)
    kept, s1, s2, s3 = call(add_kernel, [RAY] * 4, [mine, got])
    return kept, shift(s1, "tile_0", 1), shift(s2, "tile_0", 2), shift(s3, "tile_0", 3)


def to_everyone(own):
    column = [own] + [shift(own, "tile_0", -r) for r in (1, 2, 3)]
    return column + [shift(block, "tile_1", 1) for block in column]


def over_all(rows):
    return lax.all_to_all(rows, TILE + SLAB, 0, 0, tiled=True)


def shards(volume, measured, weights, footprints, foot_pixel, foot_strip):
    me = jnp.stack([lax.axis_index("tile_0"), lax.axis_index("tile_1")])
    spots = [foot_pixel, foot_strip, me]
    slabs = lax.axis_size(SLAB)
    place_in = lax.axis_index(SLAB)
    ends = jnp.stack([place_in == 0, place_in == slabs - 1]).astype(jnp.int32)
    up = [(i, (i + 1) % slabs) for i in range(slabs)]
    down = [(j, i) for i, j in up]

    field, tile = (32, 32, 128), (1, 8, 128)
    scratch = [pltpu.VMEM(field, BF16), pltpu.VMEM(field, BF16), pltpu.VMEM((64, 32, 128), F32)]
    in_place = [pltpu.with_memory_space_constraint(x, pltpu.HBM) for x in (foot_pixel, foot_strip, footprints, volume)]
    streams = [
        pltpu.VMEM(footprints.shape, F32),
        pltpu.VMEM(volume.shape, F32),
        *scratch,
        pltpu.SMEM(foot_pixel.shape, jnp.int32),
        pltpu.SMEM(foot_strip.shape, jnp.int32),
        pltpu.SemaphoreType.DMA((3,)),
        pltpu.SemaphoreType.DMA((CHUNKS,)),
    ]
    split = jax.ShapeDtypeStruct((64, 128, 256), BF16)
    half, edge = (4,) + RAY, (32, 8, 128)
    mine, theirs, first0, last0, plain, turned = call(
        first_kernel,
        [half, half, edge, edge, split, split],
        [*in_place[:2], me, *in_place[2:]],
        streams,
        3,
        any_at=(0, 1, 3, 4),
        limit=32,
    )
    parts = summed_by_owner(mine, theirs)
    residual, sent = call(start_kernel, [RAY, RAY], [*parts, measured, weights])

    mine, theirs, grad, norm0 = call(
        second_kernel, [half, half, field, tile], [*spots, plain, turned, *to_everyone(sent)], scratch, 3
    )
    mine, theirs, first0, last0 = lax.optimization_barrier((mine, theirs, first0, last0))
    parts = summed_by_owner(mine, theirs)
    first0, last0 = lax.ppermute(first0, SLAB, down), lax.ppermute(last0, SLAB, up)
    parts, first0, last0 = lax.optimization_barrier((parts, first0, last0))
    p0, sent, curve0 = call(middle_kernel, [RAY, RAY, tile], [*parts, weights])

    mine, theirs, back, crossed, first, last = call(
        third_kernel,
        [half, half, field, (2, 8, 128), edge, edge],
        [*spots, plain, turned, *to_everyone(sent), grad],
        scratch,
        3,
    )
    parts = summed_by_owner(mine, theirs)
    first, last = lax.ppermute(first, SLAB, down), lax.ppermute(last, SLAB, up)
    everyone = slabs * lax.axis_size(TILE)
    q0, rows = call(
        end_kernel, [RAY, (everyone, 128)], [*parts, weights, p0, norm0, curve0, crossed]
    )
    rows, first, last, ends = lax.optimization_barrier((rows, first, last, ends))
    rows = over_all(rows)
    alphas, again = pl.pallas_call(
        judge_kernel,
        out_shape=[jax.ShapeDtypeStruct((2,), F32), jax.ShapeDtypeStruct((1,), jnp.int32)],
        in_specs=[VM],
        out_specs=[SM, SM],
        compiler_params=pltpu.CompilerParams(vmem_limit_bytes=8 << 20),
    )(rows)

    def summed_again(alphas):
        rows = call(again_kernel, [(everyone, 128)], [alphas, weights, p0, q0, grad, back], (), 1)[0]
        return pl.pallas_call(
            ratio_kernel,
            out_shape=jax.ShapeDtypeStruct((2,), F32),
            in_specs=[SM, VM],
            out_specs=SM,
            compiler_params=pltpu.CompilerParams(vmem_limit_bytes=8 << 20),
        )(alphas, over_all(rows))

    alphas = lax.cond(again[0] == 1, summed_again, lambda known: known, alphas)
    return call(
        smooth_kernel,
        [volume.shape, measured.shape],
        [ends, alphas, volume, grad, back, first0, last0, first, last, residual, p0, q0],
        (),
        2,
    )


def solution(mesh):
    finer = Mesh(mesh.devices.reshape(4, 2, 4, 4), ("tile_0", "tile_1", "slab_0", "slab_1"))
    return jax.shard_map(
        lambda *args: tuple(shards(*args)),
        mesh=finer,
        in_specs=(
            P(SLAB, TILE),
            P(SLAB, TILE),
            P(SLAB, TILE),
            P(TILE, None, None),
            P(TILE),
            P(TILE),
        ),
        out_specs=(P(SLAB, TILE), P(SLAB, TILE)),
        check_vma=False,
    )
```

```python
import jax
import jax.numpy as jnp
from jax import lax
from jax.experimental import pallas as pl
from jax.experimental.pallas import tpu as pltpu
from jax.sharding import Mesh
from jax.sharding import PartitionSpec as P


PASSES = 3
TILE = ("tile_0", "tile_1")
SLAB = ("slab_0", "slab_1")
GROUP = 4
UNROLL = 32
CHUNKS = 4

huber_width = 0.5
smooth_rate = 0.2


VM = pl.BlockSpec(memory_space=pltpu.VMEM)
SM = pl.BlockSpec(memory_space=pltpu.SMEM)
AN = pl.BlockSpec(memory_space=pltpu.HBM)
F32 = jnp.float32
BF16 = jnp.bfloat16


def call(kernel, outs, ins, scratch=(), smem=0, flops=1000000, limit=24, any_at=()):
    specs = [AN if n in any_at else SM if n < smem else VM for n in range(len(ins))]
    return pl.pallas_call(
        kernel,
        out_shape=[s if hasattr(s, "dtype") else jax.ShapeDtypeStruct(s, F32) for s in outs],
        in_specs=specs,
        out_specs=[VM] * len(outs),
        scratch_shapes=list(scratch),
        compiler_params=pltpu.CompilerParams(vmem_limit_bytes=limit << 20),
        cost_estimate=pl.CostEstimate(flops=flops, bytes_accessed=1 << 20, transcendentals=0),
    )(*ins)


def halves(value):
    high = value.astype(BF16)
    return high, (value - high.astype(F32)).astype(BF16)


def lane_groups(shape):
    return lax.broadcasted_iota(jnp.int32, shape, 1) // 32


def place(spots, b):
    pixels, strips, me = spots
    strip = strips[b]
    owner = strip >> 5
    slot = (((owner & 1) ^ me[1]) << 2) | (((owner >> 1) - me[0]) & 3)
    return (slot << 3) | ((strip >> 2) & 7), strip & 3, pixels[b]


def stacked(pair):
    high = pair[:, :128]
    return jnp.concatenate([pair, jnp.concatenate([high, jnp.zeros_like(high)], axis=1)], axis=0)


def forward_step(spots, g, pair, high, low, rays, groups):
    where = [place(spots, GROUP * g + i) for i in range(GROUP)]
    left = jnp.concatenate([jnp.concatenate([high[w[2]], low[w[2]]], axis=1) for w in where], axis=0)
    both = lax.dot_general(left, stacked(pair), (((1,), (0,)), ((), ())), preferred_element_type=F32)
    product = both[:, :128] + both[:, 128:]
    for i, (entry, spot, _) in enumerate(where):
        own = jnp.where(groups == i, product[32 * i : 32 * i + 32], 0.0)
        rays[entry] += pltpu.roll(own, ((spot - i) & 3) * 32, 1)


def forward_loop(spots, turned, high, low, rays):
    rays[...] = jnp.zeros_like(rays)
    groups = lane_groups((32, 128))

    def step(g, carry):
        forward_step(spots, g, turned[g], high, low, rays, groups)
        return carry

    lax.fori_loop(0, turned.shape[0], step, 0, unroll=UNROLL)


def back_loop(spots, plain, rays, field):
    field[...] = jnp.zeros_like(field)
    groups = lane_groups((32, 128))

    def step(g, carry):
        where = [place(spots, GROUP * g + i) for i in range(GROUP)]
        rows = []
        for i, (entry, spot, _) in enumerate(where):
            turned = pltpu.roll(rays[entry], ((i - spot) & 3) * 32, 1)
            own = jnp.where(groups == i, turned, 0.0)
            rows.append(jnp.concatenate(halves(own), axis=1))
        left = jnp.concatenate(rows, axis=0)
        both = lax.dot_general(
            left, stacked(plain[g]), (((1,), (0,)), ((), ())), preferred_element_type=F32
        )
        product = both[:, :128] + both[:, 128:]
        for i, (_, _, pixel) in enumerate(where):
            field[pixel] += product[32 * i : 32 * i + 32]
        return carry

    lax.fori_loop(0, plain.shape[0], step, 0, unroll=UNROLL)


def hand_out(rays, mine, theirs):
    mine[...] = rays[:32].reshape(mine.shape)
    theirs[...] = rays[32:].reshape(theirs.shape)


def in_pairs(me, first, last):
    even = me[2] == 0
    return jnp.where(even, last, first), jnp.where(even, first, last)


def first_kernel(pixels_hbm, strips_hbm, me, foot_hbm, volume_hbm, *refs):
    mine, theirs, ahead, behind, plain, turned, foot, volume, high, low, rays, pixels, strips, sem, foot_sem = refs
    spots = (pixels, strips, me)
    per = foot.shape[0] // CHUNKS

    def chunk(t):
        some = pl.ds(t * per, per)
        return pltpu.make_async_copy(foot_hbm.at[some], foot.at[some], foot_sem.at[t])

    field = pltpu.make_async_copy(volume_hbm, volume, sem.at[0])
    field.start()
    indices = [
        pltpu.make_async_copy(pixels_hbm, pixels, sem.at[1]),
        pltpu.make_async_copy(strips_hbm, strips, sem.at[2]),
    ]
    for copy in indices:
        copy.start()
    for t in range(CHUNKS):
        chunk(t).start()
    rays[...] = jnp.zeros_like(rays)
    groups = lane_groups((32, 128))
    for copy in (*indices, field):
        copy.wait()
    for p in range(high.shape[0]):
        cols = slice(128 * p, 128 * p + 128)
        high[p], low[p] = halves(volume[:, cols])
        ahead[p], behind[p] = in_pairs(me, volume[0:8, cols], volume[24:32, cols])

    def trip(t, carry):
        chunk(t).wait()
        for u in range(per // GROUP):
            g = t * (per // GROUP) + u
            block = foot[pl.ds(GROUP * g, GROUP)].reshape(GROUP * 32, 128)
            plain[g] = jnp.concatenate(halves(block), axis=1)
            pair = jnp.concatenate(halves(block.T), axis=1)
            turned[g] = pair
            forward_step(spots, g, pair, high, low, rays, groups)
        return carry

    lax.fori_loop(0, CHUNKS, trip, 0)
    hand_out(rays, mine, theirs)


def folded(value):
    return jnp.sum(value.reshape(-1, 8, 128), axis=0)


def there_and_back(spots, plain, turned, pieces, mine, theirs, field, high, low, rays):
    for slot, piece in enumerate(pieces):
        rays[8 * slot : 8 * slot + 8] = piece[...]
    back_loop(spots, plain, rays, field)
    for p in range(high.shape[0]):
        high[p], low[p] = halves(field[p])
    forward_loop(spots, turned, high, low, rays)
    hand_out(rays, mine, theirs)


def second_kernel(pixels, strips, me, plain, turned, *refs):
    pieces, (mine, theirs, field, sums, high, low, rays) = refs[:8], refs[8:]
    there_and_back((pixels, strips, me), plain, turned, pieces, mine, theirs, field, high, low, rays)
    sums[0] = folded(field[...] * field[...])


def third_kernel(pixels, strips, me, plain, turned, *refs):
    pieces, grad = refs[:8], refs[8]
    mine, theirs, field, sums, ahead, behind, high, low, rays = refs[9:]
    there_and_back((pixels, strips, me), plain, turned, pieces, mine, theirs, field, high, low, rays)
    sums[0] = folded(grad[...] * field[...])
    sums[1] = folded(field[...] * field[...])
    row = lax.broadcasted_iota(jnp.int32, (8, 128), 0)
    for p in range(field.shape[0]):
        first = jnp.where(row < 3, grad[p, 0:8], pltpu.roll(field[p, 0:8], 3, 0))
        last = jnp.where(row > 4, grad[p, 24:32], pltpu.roll(field[p, 24:32], 5, 0))
        ahead[p], behind[p] = in_pairs(me, first, last)


def add_kernel(mine, got, kept, s1, s2, s3):
    for r, out in enumerate((kept, s1, s2, s3)):
        out[...] = mine[r] + got[r]


def tile_cols(ref):
    return jnp.stack([ref[:, 128 * t : 128 * t + 128] for t in range(ref.shape[1] // 128)])


def start_kernel(kept, a, b, c, measured, weights, residual, sent):
    value = kept[...] + a[...] + b[...] + c[...] - tile_cols(measured)
    residual[...] = value
    sent[...] = tile_cols(weights) * value


def resend_kernel(kept, a, b, c, weights, sent):
    sent[...] = tile_cols(weights) * (kept[...] + a[...] + b[...] + c[...])


def middle_kernel(kept, a, b, c, sent, projected, sums):
    value = kept[...] + a[...] + b[...] + c[...]
    projected[...] = value
    sums[0] = folded(sent[...] * value)


def in_lanes(sums, shape):
    lane = lax.broadcasted_iota(jnp.int32, shape, 1)
    value = jnp.zeros(shape, F32)
    for n, part in enumerate(sums):
        value = jnp.where(lane == n, jnp.sum(part, keepdims=True), value)
    return value


def end_kernel(kept, a, b, c, weights, before, norm0, curve0, turned, projected, rows):
    value = kept[...] + a[...] + b[...] + c[...]
    weighted = tile_cols(weights) * value
    projected[...] = value
    cross = folded(weighted * before[...])
    rows[...] = in_lanes([norm0[0], curve0[0], turned[0], turned[1], cross, folded(weighted * value)], rows.shape)


def totals(rows, count):
    value = jnp.sum(rows[...], axis=0, keepdims=True)
    return [value[:, n : n + 1] for n in range(count)]


def scalar(value):
    return jnp.sum(value)


def judge_kernel(rows, alphas):
    norm0, curve0, cross_g, square_g, cross_p, square_p = totals(rows, 6)
    alpha = norm0 / curve0
    norm1 = norm0 - 2.0 * alpha * cross_g + alpha * alpha * square_g
    curve1 = curve0 - 2.0 * alpha * cross_p + alpha * alpha * square_p
    sound = (norm1 > 0.01 * norm0) & (curve1 > 0.01 * curve0)
    for square in (square_g, square_p):
        sound = sound & (square > 1e-25) & (square < 1e37)
    alphas[0] = scalar(alpha)
    alphas[1] = scalar(norm1 / curve1)
    alphas[2] = scalar(jnp.where(sound, F32(0.0), F32(1.0)))


def again_kernel(alphas, weights, p0, q0, grad, turned, rows):
    value = p0[...] - alphas[0] * q0[...]
    step = grad[...] - alphas[0] * turned[...]
    rows[...] = in_lanes([folded(step * step), folded(tile_cols(weights) * value * value)], rows.shape)


def ratio_kernel(alphas, rows, out):
    norm1, curve1 = totals(rows, 2)
    out[0] = alphas[0]
    out[1] = scalar(norm1 / curve1)
    out[2] = F32(0.0)


def smooth_kernel(ends, alphas, volume, grad, turned, ahead0, behind0, ahead, behind, residual, p0, q0, smoothed, left_over):
    alpha0, alpha1 = alphas[0], alphas[1]
    rest = residual[...] - alpha0 * p0[...] - alpha1 * (p0[...] - alpha0 * q0[...])
    for t in range(rest.shape[0]):
        left_over[:, 128 * t : 128 * t + 128] = rest[t]

    def stepped(x, g, h):
        return x - alpha0 * g - alpha1 * (g - alpha0 * h)

    def both_sides(behind, ahead):
        even = ends[2] == 1
        return jnp.where(even, behind, ahead), jnp.where(even, ahead, behind)

    row = lax.broadcasted_iota(jnp.int32, (48, 128), 0)
    open_link = ~(((row == 7) & (ends[0] == 1)) | ((row == 39) & (ends[1] == 1)))
    link = jnp.where(open_link, F32(1.0), F32(0.0))
    for p in range(grad.shape[0]):
        cols = slice(128 * p, 128 * p + 128)
        last0, first0 = both_sides(behind0[p], ahead0[p])
        last, first = both_sides(behind[p], ahead[p])
        ext = jnp.concatenate(
            [
                stepped(last0, last, pltpu.roll(last, 3, 0)),
                stepped(volume[:, cols], grad[p], turned[p]),
                stepped(first0, first, pltpu.roll(first, 5, 0)),
            ],
            axis=0,
        )
        for _ in range(PASSES):
            clipped = jnp.clip(pltpu.roll(ext, 47, 0) - ext, -huber_width, huber_width) * link
            ext = ext + smooth_rate * (clipped - pltpu.roll(clipped, 1, 0))
        smoothed[:, cols] = ext[8:40]


def shift(value, axis, by):
    n = lax.axis_size(axis)
    return lax.ppermute(value, axis, [(i, (i + by) % n) for i in range(n)])


RAY = (8, 32, 128)


def summed_by_owner(mine, theirs):
    got = shift(theirs, "tile_1", 1)
    kept, s1, s2, s3 = call(add_kernel, [RAY] * 4, [mine, got])
    return kept, shift(s1, "tile_0", 1), shift(s2, "tile_0", 2), shift(s3, "tile_0", 3)


def to_everyone(own):
    column = [own] + [shift(own, "tile_0", -r) for r in (1, 2, 3)]
    return column + [shift(block, "tile_1", 1) for block in column]


def over_all(rows):
    return lax.all_to_all(rows, TILE + SLAB, 0, 0, tiled=True)


def shards(volume, measured, weights, footprints, foot_pixel, foot_strip):
    slabs = lax.axis_size(SLAB)
    place_in = lax.axis_index(SLAB)
    me = jnp.stack([lax.axis_index("tile_0"), lax.axis_index("tile_1"), place_in & 1])
    spots = [foot_pixel, foot_strip, me]
    ends = jnp.stack([place_in == 0, place_in == slabs - 1, place_in % 2 == 0]).astype(jnp.int32)
    evens = [(i, i ^ 1) for i in range(slabs)]
    odds = [(i, min(max(((i + 1) ^ 1) - 1, 0), slabs - 1)) for i in range(slabs)]

    field, tile = (32, 32, 128), (1, 8, 128)
    scratch = [pltpu.VMEM(field, BF16), pltpu.VMEM(field, BF16), pltpu.VMEM((64, 32, 128), F32)]
    in_place = [pltpu.with_memory_space_constraint(x, pltpu.HBM) for x in (foot_pixel, foot_strip, footprints, volume)]
    streams = [
        pltpu.VMEM(footprints.shape, F32),
        pltpu.VMEM(volume.shape, F32),
        *scratch,
        pltpu.SMEM(foot_pixel.shape, jnp.int32),
        pltpu.SMEM(foot_strip.shape, jnp.int32),
        pltpu.SemaphoreType.DMA((3,)),
        pltpu.SemaphoreType.DMA((CHUNKS,)),
    ]
    split = jax.ShapeDtypeStruct((64, 128, 256), BF16)
    half, edge = (4,) + RAY, (32, 8, 128)
    mine, theirs, ahead0, behind0, plain, turned = call(
        first_kernel,
        [half, half, edge, edge, split, split],
        [*in_place[:2], me, *in_place[2:]],
        streams,
        3,
        any_at=(0, 1, 3, 4),
        limit=32,
    )
    parts = summed_by_owner(mine, theirs)
    residual, sent = call(start_kernel, [RAY, RAY], [*parts, measured, weights])

    mine, theirs, grad, norm0 = call(
        second_kernel, [half, half, field, tile], [*spots, plain, turned, *to_everyone(sent)], scratch, 3
    )
    mine, theirs, ahead0, behind0 = lax.optimization_barrier((mine, theirs, ahead0, behind0))
    parts = summed_by_owner(mine, theirs)
    ahead0, behind0 = lax.ppermute(ahead0, SLAB, evens), lax.ppermute(behind0, SLAB, odds)
    parts, ahead0, behind0 = lax.optimization_barrier((parts, ahead0, behind0))
    sent = call(resend_kernel, [RAY], [*parts, weights])[0]
    p0, curve0 = call(middle_kernel, [RAY, tile], [*parts, sent])

    mine, theirs, back, crossed, ahead, behind = call(
        third_kernel,
        [half, half, field, (2, 8, 128), edge, edge],
        [*spots, plain, turned, *to_everyone(sent), grad],
        scratch,
        3,
    )
    parts = summed_by_owner(mine, theirs)
    ahead, behind = lax.ppermute(ahead, SLAB, evens), lax.ppermute(behind, SLAB, odds)
    everyone = slabs * lax.axis_size(TILE)
    q0, rows = call(
        end_kernel, [RAY, (everyone, 128)], [*parts, weights, p0, norm0, curve0, crossed]
    )
    rows, ahead, behind, ends = lax.optimization_barrier((rows, ahead, behind, ends))
    rows = over_all(rows)
    alphas = pl.pallas_call(
        judge_kernel,
        out_shape=jax.ShapeDtypeStruct((3,), F32),
        in_specs=[VM],
        out_specs=SM,
        compiler_params=pltpu.CompilerParams(vmem_limit_bytes=8 << 20),
    )(rows)

    def summed_again(alphas):
        rows = call(again_kernel, [(everyone, 128)], [alphas, weights, p0, q0, grad, back], (), 1)[0]
        return pl.pallas_call(
            ratio_kernel,
            out_shape=jax.ShapeDtypeStruct((3,), F32),
            in_specs=[SM, VM],
            out_specs=SM,
            compiler_params=pltpu.CompilerParams(vmem_limit_bytes=8 << 20),
        )(alphas, over_all(rows))

    alphas = lax.cond(alphas[2] > 0.5, summed_again, lambda known: known, alphas)
    return call(
        smooth_kernel,
        [volume.shape, measured.shape],
        [ends, alphas, volume, grad, back, ahead0, behind0, ahead, behind, residual, p0, q0],
        (),
        2,
    )


def solution(mesh):
    finer = Mesh(mesh.devices.reshape(4, 2, 4, 4), ("tile_0", "tile_1", "slab_0", "slab_1"))
    return jax.shard_map(
        lambda *args: tuple(shards(*args)),
        mesh=finer,
        in_specs=(
            P(SLAB, TILE),
            P(SLAB, TILE),
            P(SLAB, TILE),
            P(TILE, None, None),
            P(TILE),
            P(TILE),
        ),
        out_specs=(P(SLAB, TILE), P(SLAB, TILE)),
        check_vma=False,
    )
```

```python
import jax
import jax.numpy as jnp
from jax import lax
from jax.experimental import pallas as pl
from jax.experimental.pallas import tpu as pltpu
from jax.sharding import Mesh
from jax.sharding import PartitionSpec as P


PASSES = 3
TILE = ("tile_0", "tile_1")
SLAB = ("slab_0", "slab_1")
GROUP = 4
UNROLL = 32
CHUNKS = 4

huber_width = 0.5
smooth_rate = 0.2


VM = pl.BlockSpec(memory_space=pltpu.VMEM)
SM = pl.BlockSpec(memory_space=pltpu.SMEM)
AN = pl.BlockSpec(memory_space=pltpu.HBM)
F32 = jnp.float32
BF16 = jnp.bfloat16


def call(kernel, outs, ins, scratch=(), smem=0, flops=1000000, limit=24, any_at=()):
    specs = [AN if n in any_at else SM if n < smem else VM for n in range(len(ins))]
    return pl.pallas_call(
        kernel,
        out_shape=[s if hasattr(s, "dtype") else jax.ShapeDtypeStruct(s, F32) for s in outs],
        in_specs=specs,
        out_specs=[VM] * len(outs),
        scratch_shapes=list(scratch),
        compiler_params=pltpu.CompilerParams(vmem_limit_bytes=limit << 20),
        cost_estimate=pl.CostEstimate(flops=flops, bytes_accessed=1 << 20, transcendentals=0),
    )(*ins)


def halves(value):
    high = value.astype(BF16)
    return high, (value - high.astype(F32)).astype(BF16)


def lane_groups(shape):
    return lax.broadcasted_iota(jnp.int32, shape, 1) // 32


def place(spots, b):
    pixels, strips, me = spots
    strip = strips[b]
    owner = strip >> 5
    slot = (((owner & 1) ^ me[1]) << 2) | (((owner >> 1) - me[0]) & 3)
    return (slot << 3) | ((strip >> 2) & 7), strip & 3, pixels[b]


def stacked(pair):
    high = pair[:, :128]
    return jnp.concatenate([pair, jnp.concatenate([high, jnp.zeros_like(high)], axis=1)], axis=0)


def forward_step(spots, g, pair, high, low, rays, groups):
    where = [place(spots, GROUP * g + i) for i in range(GROUP)]
    left = jnp.concatenate([jnp.concatenate([high[w[2]], low[w[2]]], axis=1) for w in where], axis=0)
    both = lax.dot_general(left, stacked(pair), (((1,), (0,)), ((), ())), preferred_element_type=F32)
    product = both[:, :128] + both[:, 128:]
    for i, (entry, spot, _) in enumerate(where):
        own = jnp.where(groups == i, product[32 * i : 32 * i + 32], 0.0)
        rays[entry] += pltpu.roll(own, ((spot - i) & 3) * 32, 1)


def forward_loop(spots, turned, high, low, rays):
    rays[...] = jnp.zeros_like(rays)
    groups = lane_groups((32, 128))

    def step(g, carry):
        forward_step(spots, g, turned[g], high, low, rays, groups)
        return carry

    lax.fori_loop(0, turned.shape[0], step, 0, unroll=UNROLL)


def back_loop(spots, plain, rays, field):
    field[...] = jnp.zeros_like(field)
    groups = lane_groups((32, 128))

    def step(g, carry):
        where = [place(spots, GROUP * g + i) for i in range(GROUP)]
        rows = []
        for i, (entry, spot, _) in enumerate(where):
            turned = pltpu.roll(rays[entry], ((i - spot) & 3) * 32, 1)
            own = jnp.where(groups == i, turned, 0.0)
            rows.append(jnp.concatenate(halves(own), axis=1))
        left = jnp.concatenate(rows, axis=0)
        both = lax.dot_general(
            left, stacked(plain[g]), (((1,), (0,)), ((), ())), preferred_element_type=F32
        )
        product = both[:, :128] + both[:, 128:]
        for i, (_, _, pixel) in enumerate(where):
            field[pixel] += product[32 * i : 32 * i + 32]
        return carry

    lax.fori_loop(0, plain.shape[0], step, 0, unroll=UNROLL)


def hand_out(rays, mine, theirs):
    mine[...] = rays[:32].reshape(mine.shape)
    theirs[...] = rays[32:].reshape(theirs.shape)


def first_kernel(pixels_hbm, strips_hbm, me, foot_hbm, volume_hbm, *refs):
    mine, theirs, first, last, plain, turned, foot, volume, high, low, rays, pixels, strips, sem, foot_sem = refs
    spots = (pixels, strips, me)
    per = foot.shape[0] // CHUNKS

    def chunk(t):
        some = pl.ds(t * per, per)
        return pltpu.make_async_copy(foot_hbm.at[some], foot.at[some], foot_sem.at[t])

    field = pltpu.make_async_copy(volume_hbm, volume, sem.at[0])
    field.start()
    indices = [
        pltpu.make_async_copy(pixels_hbm, pixels, sem.at[1]),
        pltpu.make_async_copy(strips_hbm, strips, sem.at[2]),
    ]
    for copy in indices:
        copy.start()
    for t in range(CHUNKS):
        chunk(t).start()
    rays[...] = jnp.zeros_like(rays)
    groups = lane_groups((32, 128))
    for copy in (*indices, field):
        copy.wait()
    for p in range(high.shape[0]):
        cols = slice(128 * p, 128 * p + 128)
        high[p], low[p] = halves(volume[:, cols])
        first[p], last[p] = volume[0:8, cols], volume[24:32, cols]

    def trip(t, carry):
        chunk(t).wait()
        for u in range(per // GROUP):
            g = t * (per // GROUP) + u
            block = foot[pl.ds(GROUP * g, GROUP)].reshape(GROUP * 32, 128)
            plain[g] = jnp.concatenate(halves(block), axis=1)
            pair = jnp.concatenate(halves(block.T), axis=1)
            turned[g] = pair
            forward_step(spots, g, pair, high, low, rays, groups)
        return carry

    lax.fori_loop(0, CHUNKS, trip, 0)
    hand_out(rays, mine, theirs)


def folded(value):
    return jnp.sum(value.reshape(-1, 8, 128), axis=0)


def there_and_back(spots, plain, turned, pieces, mine, theirs, field, high, low, rays):
    for slot, piece in enumerate(pieces):
        rays[8 * slot : 8 * slot + 8] = piece[...]
    back_loop(spots, plain, rays, field)
    for p in range(high.shape[0]):
        high[p], low[p] = halves(field[p])
    forward_loop(spots, turned, high, low, rays)
    hand_out(rays, mine, theirs)


def second_kernel(pixels, strips, me, plain, turned, *refs):
    pieces, (mine, theirs, field, sums, high, low, rays) = refs[:8], refs[8:]
    there_and_back((pixels, strips, me), plain, turned, pieces, mine, theirs, field, high, low, rays)
    sums[0] = folded(field[...] * field[...])


def third_kernel(pixels, strips, me, plain, turned, *refs):
    pieces, grad = refs[:8], refs[8]
    mine, theirs, field, sums, first, last, high, low, rays = refs[9:]
    there_and_back((pixels, strips, me), plain, turned, pieces, mine, theirs, field, high, low, rays)
    sums[0] = folded(grad[...] * field[...])
    sums[1] = folded(field[...] * field[...])
    row = lax.broadcasted_iota(jnp.int32, (8, 128), 0)
    for p in range(field.shape[0]):
        first[p] = jnp.where(row < 3, grad[p, 0:8], pltpu.roll(field[p, 0:8], 3, 0))
        last[p] = jnp.where(row > 4, grad[p, 24:32], pltpu.roll(field[p, 24:32], 5, 0))


def add_kernel(mine, got, kept, s1, s2, s3):
    for r, out in enumerate((kept, s1, s2, s3)):
        out[...] = mine[r] + got[r]


def tile_cols(ref):
    return jnp.stack([ref[:, 128 * t : 128 * t + 128] for t in range(ref.shape[1] // 128)])


def start_kernel(kept, a, b, c, measured, weights, residual, sent):
    value = kept[...] + a[...] + b[...] + c[...] - tile_cols(measured)
    residual[...] = value
    sent[...] = tile_cols(weights) * value


def resend_kernel(kept, a, b, c, weights, sent):
    sent[...] = tile_cols(weights) * (kept[...] + a[...] + b[...] + c[...])


def middle_kernel(kept, a, b, c, sent, projected, sums):
    value = kept[...] + a[...] + b[...] + c[...]
    projected[...] = value
    sums[0] = folded(sent[...] * value)


def in_lanes(sums, shape):
    lane = lax.broadcasted_iota(jnp.int32, shape, 1)
    value = jnp.zeros(shape, F32)
    for n, part in enumerate(sums):
        value = jnp.where(lane == n, jnp.sum(part, keepdims=True), value)
    return value


def end_kernel(kept, a, b, c, weights, before, norm0, curve0, turned, projected, rows):
    value = kept[...] + a[...] + b[...] + c[...]
    weighted = tile_cols(weights) * value
    projected[...] = value
    cross = folded(weighted * before[...])
    rows[...] = in_lanes([norm0[0], curve0[0], turned[0], turned[1], cross, folded(weighted * value)], rows.shape)


def totals(rows, count):
    value = jnp.sum(rows[...], axis=0, keepdims=True)
    return [value[:, n : n + 1] for n in range(count)]


def scalar(value):
    return jnp.sum(value)


def judge_kernel(rows, alphas, again):
    norm0, curve0, cross_g, square_g, cross_p, square_p = totals(rows, 6)
    alpha = norm0 / curve0
    norm1 = norm0 - 2.0 * alpha * cross_g + alpha * alpha * square_g
    curve1 = curve0 - 2.0 * alpha * cross_p + alpha * alpha * square_p
    sound = (norm1 > 0.01 * norm0) & (curve1 > 0.01 * curve0)
    for square in (square_g, square_p):
        sound = sound & (square > 1e-25) & (square < 1e37)
    alphas[0] = scalar(alpha)
    alphas[1] = scalar(norm1 / curve1)
    again[0] = jnp.where(scalar(jnp.where(sound, F32(0.0), F32(1.0))) > 0.5, 1, 0)


def again_kernel(alphas, weights, p0, q0, grad, turned, rows):
    value = p0[...] - alphas[0] * q0[...]
    step = grad[...] - alphas[0] * turned[...]
    rows[...] = in_lanes([folded(step * step), folded(tile_cols(weights) * value * value)], rows.shape)


def ratio_kernel(alphas, rows, out):
    norm1, curve1 = totals(rows, 2)
    out[0] = alphas[0]
    out[1] = scalar(norm1 / curve1)


def smooth_kernel(ends, alphas, volume, grad, turned, first0, last0, first, last, residual, p0, q0, smoothed, left_over):
    alpha0, alpha1 = alphas[0], alphas[1]
    rest = residual[...] - alpha0 * p0[...] - alpha1 * (p0[...] - alpha0 * q0[...])
    for t in range(rest.shape[0]):
        left_over[:, 128 * t : 128 * t + 128] = rest[t]

    def stepped(x, g, h):
        return x - alpha0 * g - alpha1 * (g - alpha0 * h)

    row = lax.broadcasted_iota(jnp.int32, (48, 128), 0)
    open_link = ~(((row == 7) & (ends[0] == 1)) | ((row == 39) & (ends[1] == 1)))
    link = jnp.where(open_link, F32(1.0), F32(0.0))
    for p in range(grad.shape[0]):
        cols = slice(128 * p, 128 * p + 128)
        ext = jnp.concatenate(
            [
                stepped(last0[p], last[p], pltpu.roll(last[p], 3, 0)),
                stepped(volume[:, cols], grad[p], turned[p]),
                stepped(first0[p], first[p], pltpu.roll(first[p], 5, 0)),
            ],
            axis=0,
        )
        for _ in range(PASSES):
            clipped = jnp.clip(pltpu.roll(ext, 47, 0) - ext, -huber_width, huber_width) * link
            ext = ext + smooth_rate * (clipped - pltpu.roll(clipped, 1, 0))
        smoothed[:, cols] = ext[8:40]


def shift(value, axis, by):
    n = lax.axis_size(axis)
    return lax.ppermute(value, axis, [(i, (i + by) % n) for i in range(n)])


RAY = (8, 32, 128)


def summed_by_owner(mine, theirs):
    got = shift(theirs, "tile_1", 1)
    kept, s1, s2, s3 = call(add_kernel, [RAY] * 4, [mine, got])
    return kept, shift(s1, "tile_0", 1), shift(s2, "tile_0", 2), shift(s3, "tile_0", 3)


def to_everyone(own):
    column = [own] + [shift(own, "tile_0", -r) for r in (1, 2, 3)]
    return column + [shift(block, "tile_1", 1) for block in column]


def over_all(rows):
    return lax.all_to_all(rows, TILE + SLAB, 0, 0, tiled=True)


def shards(volume, measured, weights, footprints, foot_pixel, foot_strip):
    me = jnp.stack([lax.axis_index("tile_0"), lax.axis_index("tile_1")])
    spots = [foot_pixel, foot_strip, me]
    slabs = lax.axis_size(SLAB)
    place_in = lax.axis_index(SLAB)
    ends = jnp.stack([place_in == 0, place_in == slabs - 1]).astype(jnp.int32)
    up = [(i, (i + 1) % slabs) for i in range(slabs)]
    down = [(j, i) for i, j in up]

    field, tile = (32, 32, 128), (1, 8, 128)
    scratch = [pltpu.VMEM(field, BF16), pltpu.VMEM(field, BF16), pltpu.VMEM((64, 32, 128), F32)]
    in_place = [pltpu.with_memory_space_constraint(x, pltpu.HBM) for x in (foot_pixel, foot_strip, footprints, volume)]
    streams = [
        pltpu.VMEM(footprints.shape, F32),
        pltpu.VMEM(volume.shape, F32),
        *scratch,
        pltpu.SMEM(foot_pixel.shape, jnp.int32),
        pltpu.SMEM(foot_strip.shape, jnp.int32),
        pltpu.SemaphoreType.DMA((3,)),
        pltpu.SemaphoreType.DMA((CHUNKS,)),
    ]
    split = jax.ShapeDtypeStruct((64, 128, 256), BF16)
    half, edge = (4,) + RAY, (32, 8, 128)
    mine, theirs, first0, last0, plain, turned = call(
        first_kernel,
        [half, half, edge, edge, split, split],
        [*in_place[:2], me, *in_place[2:]],
        streams,
        3,
        any_at=(0, 1, 3, 4),
        limit=32,
    )
    parts = summed_by_owner(mine, theirs)
    residual, sent = call(start_kernel, [RAY, RAY], [*parts, measured, weights])

    mine, theirs, grad, norm0 = call(
        second_kernel, [half, half, field, tile], [*spots, plain, turned, *to_everyone(sent)], scratch, 3
    )
    mine, theirs, first0, last0 = lax.optimization_barrier((mine, theirs, first0, last0))
    parts = summed_by_owner(mine, theirs)
    first0, last0 = lax.ppermute(first0, SLAB, down), lax.ppermute(last0, SLAB, up)
    sent = call(resend_kernel, [RAY], [*parts, weights])[0]
    p0, curve0 = call(middle_kernel, [RAY, tile], [*parts, sent])
    pieces = to_everyone(sent)
    pieces, first0, last0 = lax.optimization_barrier((pieces, first0, last0))

    mine, theirs, back, crossed, first, last = call(
        third_kernel,
        [half, half, field, (2, 8, 128), edge, edge],
        [*spots, plain, turned, *pieces, grad],
        scratch,
        3,
    )
    parts = summed_by_owner(mine, theirs)
    first, last = lax.ppermute(first, SLAB, down), lax.ppermute(last, SLAB, up)
    everyone = slabs * lax.axis_size(TILE)
    q0, rows = call(
        end_kernel, [RAY, (everyone, 128)], [*parts, weights, p0, norm0, curve0, crossed]
    )
    rows, ends = lax.optimization_barrier((rows, ends))
    rows = over_all(rows)
    alphas, again = pl.pallas_call(
        judge_kernel,
        out_shape=[jax.ShapeDtypeStruct((2,), F32), jax.ShapeDtypeStruct((1,), jnp.int32)],
        in_specs=[VM],
        out_specs=[SM, SM],
        compiler_params=pltpu.CompilerParams(vmem_limit_bytes=8 << 20),
    )(rows)

    def summed_again(alphas):
        rows = call(again_kernel, [(everyone, 128)], [alphas, weights, p0, q0, grad, back], (), 1)[0]
        return pl.pallas_call(
            ratio_kernel,
            out_shape=jax.ShapeDtypeStruct((2,), F32),
            in_specs=[SM, VM],
            out_specs=SM,
            compiler_params=pltpu.CompilerParams(vmem_limit_bytes=8 << 20),
        )(alphas, over_all(rows))

    alphas = lax.cond(again[0] == 1, summed_again, lambda known: known, alphas)
    return call(
        smooth_kernel,
        [volume.shape, measured.shape],
        [ends, alphas, volume, grad, back, first0, last0, first, last, residual, p0, q0],
        (),
        2,
    )


def solution(mesh):
    finer = Mesh(mesh.devices.reshape(4, 2, 4, 4), ("tile_0", "tile_1", "slab_0", "slab_1"))
    return jax.shard_map(
        lambda *args: tuple(shards(*args)),
        mesh=finer,
        in_specs=(
            P(SLAB, TILE),
            P(SLAB, TILE),
            P(SLAB, TILE),
            P(TILE, None, None),
            P(TILE),
            P(TILE),
        ),
        out_specs=(P(SLAB, TILE), P(SLAB, TILE)),
        check_vma=False,
    )
```

```python
import jax
import jax.numpy as jnp
from jax import lax
from jax.experimental import pallas as pl
from jax.experimental.pallas import tpu as pltpu
from jax.sharding import Mesh
from jax.sharding import PartitionSpec as P


PASSES = 3
TILE = ("tile_0", "tile_1")
SLAB = ("slab_0", "slab_1")
GROUP = 4
UNROLL = 64
CHUNKS = 4

huber_width = 0.5
smooth_rate = 0.2


VM = pl.BlockSpec(memory_space=pltpu.VMEM)
SM = pl.BlockSpec(memory_space=pltpu.SMEM)
AN = pl.BlockSpec(memory_space=pltpu.HBM)
F32 = jnp.float32
BF16 = jnp.bfloat16


def call(kernel, outs, ins, scratch=(), smem=0, flops=1000000, limit=10, any_at=()):
    specs = [AN if n in any_at else SM if n < smem else VM for n in range(len(ins))]
    return pl.pallas_call(
        kernel,
        out_shape=[s if hasattr(s, "dtype") else jax.ShapeDtypeStruct(s, F32) for s in outs],
        in_specs=specs,
        out_specs=[VM] * len(outs),
        scratch_shapes=list(scratch),
        compiler_params=pltpu.CompilerParams(vmem_limit_bytes=limit << 20),
        cost_estimate=pl.CostEstimate(flops=flops, bytes_accessed=1 << 20, transcendentals=0),
    )(*ins)


def halves(value):
    high = value.astype(BF16)
    return high, (value - high.astype(F32)).astype(BF16)


def lane_groups(shape):
    return lax.broadcasted_iota(jnp.int32, shape, 1) // 32


def place(spots, b):
    pixels, strips, me = spots
    strip = strips[b]
    owner = strip >> 5
    slot = (((owner & 1) ^ me[1]) << 2) | (((owner >> 1) - me[0]) & 3)
    return (slot << 3) | ((strip >> 2) & 7), strip & 3, pixels[b]


def stacked(pair):
    high = pair[:, :128]
    return jnp.concatenate([pair, jnp.concatenate([high, jnp.zeros_like(high)], axis=1)], axis=0)


def forward_step(spots, g, pair, high, low, rays, groups):
    where = [place(spots, GROUP * g + i) for i in range(GROUP)]
    left = jnp.concatenate([jnp.concatenate([high[w[2]], low[w[2]]], axis=1) for w in where], axis=0)
    both = lax.dot_general(left, stacked(pair), (((1,), (0,)), ((), ())), preferred_element_type=F32)
    product = both[:, :128] + both[:, 128:]
    for i, (entry, spot, _) in enumerate(where):
        own = jnp.where(groups == i, product[32 * i : 32 * i + 32], 0.0)
        rays[entry] += pltpu.roll(own, ((spot - i) & 3) * 32, 1)


def forward_loop(spots, turned, high, low, rays):
    rays[...] = jnp.zeros_like(rays)
    groups = lane_groups((32, 128))

    def step(g, carry):
        forward_step(spots, g, turned[g], high, low, rays, groups)
        return carry

    lax.fori_loop(0, turned.shape[0], step, 0, unroll=UNROLL)


def back_loop(spots, plain, rays, field):
    field[...] = jnp.zeros_like(field)
    groups = lane_groups((32, 128))

    def step(g, carry):
        where = [place(spots, GROUP * g + i) for i in range(GROUP)]
        rows = []
        for i, (entry, spot, _) in enumerate(where):
            turned = pltpu.roll(rays[entry], ((i - spot) & 3) * 32, 1)
            own = jnp.where(groups == i, turned, 0.0)
            rows.append(jnp.concatenate(halves(own), axis=1))
        left = jnp.concatenate(rows, axis=0)
        both = lax.dot_general(
            left, stacked(plain[g]), (((1,), (0,)), ((), ())), preferred_element_type=F32
        )
        product = both[:, :128] + both[:, 128:]
        for i, (_, _, pixel) in enumerate(where):
            field[pixel] += product[32 * i : 32 * i + 32]
        return carry

    lax.fori_loop(0, plain.shape[0], step, 0, unroll=UNROLL)


def hand_out(rays, mine, theirs):
    mine[...] = rays[:32].reshape(mine.shape)
    theirs[...] = rays[32:].reshape(theirs.shape)


def first_kernel(pixels_hbm, strips_hbm, me, foot_hbm, volume_hbm, *refs):
    mine, theirs, first, last, plain, turned, foot, volume, high, low, rays, pixels, strips, sem, foot_sem = refs
    spots = (pixels, strips, me)
    per = foot.shape[0] // CHUNKS

    def chunk(t):
        some = pl.ds(t * per, per)
        return pltpu.make_async_copy(foot_hbm.at[some], foot.at[some], foot_sem.at[t])

    field = pltpu.make_async_copy(volume_hbm, volume, sem.at[0])
    field.start()
    indices = [
        pltpu.make_async_copy(pixels_hbm, pixels, sem.at[1]),
        pltpu.make_async_copy(strips_hbm, strips, sem.at[2]),
    ]
    for copy in indices:
        copy.start()
    for t in range(CHUNKS):
        chunk(t).start()
    rays[...] = jnp.zeros_like(rays)
    groups = lane_groups((32, 128))
    for copy in (*indices, field):
        copy.wait()
    for p in range(high.shape[0]):
        cols = slice(128 * p, 128 * p + 128)
        high[p], low[p] = halves(volume[:, cols])
        first[p], last[p] = volume[0:8, cols], volume[24:32, cols]

    def trip(t, carry):
        chunk(t).wait()
        for u in range(per // GROUP):
            g = t * (per // GROUP) + u
            block = foot[pl.ds(GROUP * g, GROUP)].reshape(GROUP * 32, 128)
            plain[g] = jnp.concatenate(halves(block), axis=1)
            pair = jnp.concatenate(halves(block.T), axis=1)
            turned[g] = pair
            forward_step(spots, g, pair, high, low, rays, groups)
        return carry

    lax.fori_loop(0, CHUNKS, trip, 0)
    hand_out(rays, mine, theirs)


def folded(value):
    return jnp.sum(value.reshape(-1, 8, 128), axis=0)


def there_and_back(spots, plain, turned, pieces, mine, theirs, field, high, low, rays):
    for slot, piece in enumerate(pieces):
        rays[8 * slot : 8 * slot + 8] = piece[...]
    back_loop(spots, plain, rays, field)
    for p in range(high.shape[0]):
        high[p], low[p] = halves(field[p])
    forward_loop(spots, turned, high, low, rays)
    hand_out(rays, mine, theirs)


def two_firsts(one, other):
    row = lax.broadcasted_iota(jnp.int32, (8, 128), 0)
    return jnp.where(row < 3, one, pltpu.roll(other, 3, 0))


def two_lasts(one, other):
    row = lax.broadcasted_iota(jnp.int32, (8, 128), 0)
    return jnp.where(row > 4, one, pltpu.roll(other, 5, 0))


def second_kernel(pixels, strips, me, plain, turned, *refs):
    pieces, first0, last0 = refs[:8], refs[8], refs[9]
    mine, theirs, field, sums, first, last, high, low, rays = refs[10:]
    there_and_back((pixels, strips, me), plain, turned, pieces, mine, theirs, field, high, low, rays)
    sums[0] = folded(field[...] * field[...])
    for p in range(field.shape[0]):
        first[p] = two_firsts(first0[p], field[p, 0:8])
        last[p] = two_lasts(last0[p], field[p, 24:32])


def third_kernel(pixels, strips, me, plain, turned, *refs):
    pieces, grad = refs[:8], refs[8]
    mine, theirs, field, sums, first, last, high, low, rays = refs[9:]
    there_and_back((pixels, strips, me), plain, turned, pieces, mine, theirs, field, high, low, rays)
    sums[0] = folded(grad[...] * field[...])
    sums[1] = folded(field[...] * field[...])
    for q in range(first.shape[0]):
        one, other = field[2 * q], field[2 * q + 1]
        first[q] = two_firsts(one[0:8], other[0:8])
        last[q] = two_lasts(one[24:32], other[24:32])


def add_kernel(mine, got, kept, s1, s2, s3):
    for r, out in enumerate((kept, s1, s2, s3)):
        out[...] = mine[r] + got[r]


def tile_cols(ref):
    return jnp.stack([ref[:, 128 * t : 128 * t + 128] for t in range(ref.shape[1] // 128)])


def start_kernel(kept, a, b, c, measured, weights, residual, sent):
    value = kept[...] + a[...] + b[...] + c[...] - tile_cols(measured)
    residual[...] = value
    sent[...] = tile_cols(weights) * value


def resend_kernel(kept, a, b, c, weights, sent):
    sent[...] = tile_cols(weights) * (kept[...] + a[...] + b[...] + c[...])


def middle_kernel(kept, a, b, c, sent, back, projected, sums, spare):
    spare[...] = back[...]
    value = kept[...] + a[...] + b[...] + c[...]
    projected[...] = value
    sums[0] = folded(sent[...] * value)


SPAN = 16


def in_lanes(sums, shape):
    rows = [jnp.sum(part, axis=0, keepdims=True) for part in sums]
    rows += [jnp.zeros((1, 128), F32)] * (8 - len(rows))
    value = jnp.concatenate(rows, axis=0)
    for by in (64, 32, 16):
        value = value + pltpu.roll(value, by, 1)
    own = lax.broadcasted_iota(jnp.int32, (8, 128), 0) == lax.broadcasted_iota(jnp.int32, (8, 128), 1) // SPAN
    return jnp.broadcast_to(jnp.sum(jnp.where(own, value, 0.0), axis=0, keepdims=True), shape)


def end_kernel(kept, a, b, c, weights, before, norm0, curve0, turned, projected, rows):
    value = kept[...] + a[...] + b[...] + c[...]
    weighted = tile_cols(weights) * value
    projected[...] = value
    cross = folded(weighted * before[...])
    rows[...] = in_lanes([norm0[0], curve0[0], turned[0], turned[1], cross, folded(weighted * value)], rows.shape)


def totals(rows, count):
    value = jnp.sum(rows[...], axis=0, keepdims=True)
    group = lax.broadcasted_iota(jnp.int32, value.shape, 1) // SPAN
    return [jnp.sum(jnp.where(group == n, value, 0.0), axis=1, keepdims=True) for n in range(count)]


def scalar(value):
    return jnp.sum(value)


def judge_kernel(rows, alphas, again):
    norm0, curve0, cross_g, square_g, cross_p, square_p = totals(rows, 6)
    alpha = norm0 / curve0
    norm1 = norm0 - 2.0 * alpha * cross_g + alpha * alpha * square_g
    curve1 = curve0 - 2.0 * alpha * cross_p + alpha * alpha * square_p
    sound = (norm1 > 0.01 * norm0) & (curve1 > 0.01 * curve0)
    for square in (square_g, square_p):
        sound = sound & (square > 1e-25) & (square < 1e37)
    alphas[0] = scalar(alpha)
    alphas[1] = scalar(norm1 / curve1)
    again[0] = jnp.where(scalar(jnp.where(sound, F32(0.0), F32(1.0))) > 0.5, 1, 0)


def again_kernel(alphas, weights, p0, q0, grad, turned, rows):
    value = p0[...] - alphas[0] * q0[...]
    step = grad[...] - alphas[0] * turned[...]
    rows[...] = in_lanes([folded(step * step), folded(tile_cols(weights) * value * value)], rows.shape)


def ratio_kernel(alphas, rows, out):
    norm1, curve1 = totals(rows, 2)
    out[0] = alphas[0]
    out[1] = scalar(norm1 / curve1)


def smooth_kernel(ends, alphas, volume, grad, turned, first0, last0, first, last, residual, p0, q0, smoothed, left_over):
    alpha0, alpha1 = alphas[0], alphas[1]
    rest = residual[...] - alpha0 * p0[...] - alpha1 * (p0[...] - alpha0 * q0[...])
    for t in range(rest.shape[0]):
        left_over[:, 128 * t : 128 * t + 128] = rest[t]

    def stepped(x, g, h):
        return x - alpha0 * g - alpha1 * (g - alpha0 * h)

    row = lax.broadcasted_iota(jnp.int32, (48, 128), 0)
    open_link = ~(((row == 7) & (ends[0] == 1)) | ((row == 39) & (ends[1] == 1)))
    link = jnp.where(open_link, F32(1.0), F32(0.0))
    for p in range(grad.shape[0]):
        cols = slice(128 * p, 128 * p + 128)
        last_h, first_h = last[p // 2], first[p // 2]
        if p % 2:
            last_h, first_h = pltpu.roll(last_h, 3, 0), pltpu.roll(first_h, 5, 0)
        ext = jnp.concatenate(
            [
                stepped(last0[p], pltpu.roll(last0[p], 3, 0), last_h),
                stepped(volume[:, cols], grad[p], turned[p]),
                stepped(first0[p], pltpu.roll(first0[p], 5, 0), first_h),
            ],
            axis=0,
        )
        for _ in range(PASSES):
            clipped = jnp.clip(pltpu.roll(ext, 47, 0) - ext, -huber_width, huber_width) * link
            ext = ext + smooth_rate * (clipped - pltpu.roll(clipped, 1, 0))
        smoothed[:, cols] = ext[8:40]


def shift(value, axis, by):
    n = lax.axis_size(axis)
    return lax.ppermute(value, axis, [(i, (i + by) % n) for i in range(n)])


RAY = (8, 32, 128)


def summed_by_owner(mine, theirs):
    got = shift(theirs, "tile_1", 1)
    kept, s1, s2, s3 = call(add_kernel, [RAY] * 4, [mine, got])
    return kept, shift(s1, "tile_0", 1), shift(s2, "tile_0", 2), shift(s3, "tile_0", 3)


def to_everyone(own):
    column = [own] + [shift(own, "tile_0", -r) for r in (1, 2, 3)]
    return column + [shift(block, "tile_1", 1) for block in column]


def over_all(rows):
    return lax.all_to_all(rows, TILE + SLAB, 0, 0, tiled=True)


def shards(volume, measured, weights, footprints, foot_pixel, foot_strip):
    me = jnp.stack([lax.axis_index("tile_0"), lax.axis_index("tile_1")])
    spots = [foot_pixel, foot_strip, me]
    slabs = lax.axis_size(SLAB)
    place_in = lax.axis_index(SLAB)
    ends = jnp.stack([place_in == 0, place_in == slabs - 1]).astype(jnp.int32)
    up = [(i, (i + 1) % slabs) for i in range(slabs)]
    down = [(j, i) for i, j in up]

    field, tile = (32, 32, 128), (1, 8, 128)
    scratch = [pltpu.VMEM(field, BF16), pltpu.VMEM(field, BF16), pltpu.VMEM((64, 32, 128), F32)]
    in_place = [pltpu.with_memory_space_constraint(x, pltpu.HBM) for x in (foot_pixel, foot_strip, footprints, volume)]
    streams = [
        pltpu.VMEM(footprints.shape, F32),
        pltpu.VMEM(volume.shape, F32),
        *scratch,
        pltpu.SMEM(foot_pixel.shape, jnp.int32),
        pltpu.SMEM(foot_strip.shape, jnp.int32),
        pltpu.SemaphoreType.DMA((3,)),
        pltpu.SemaphoreType.DMA((CHUNKS,)),
    ]
    split = jax.ShapeDtypeStruct((64, 128, 256), BF16)
    half, edge = (4,) + RAY, (32, 8, 128)
    mine, theirs, first0, last0, plain, turned = call(
        first_kernel,
        [half, half, edge, edge, split, split],
        [*in_place[:2], me, *in_place[2:]],
        streams,
        3,
        any_at=(0, 1, 3, 4),
        limit=16,
    )
    parts = summed_by_owner(mine, theirs)
    residual, sent = call(start_kernel, [RAY, RAY], [*parts, measured, weights])

    mine, theirs, grad, norm0, first0, last0 = call(
        second_kernel,
        [half, half, field, tile, edge, edge],
        [*spots, plain, turned, *to_everyone(sent), first0, last0],
        scratch,
        3,
    )
    parts = summed_by_owner(mine, theirs)
    first0, last0 = lax.ppermute(first0, SLAB, down), lax.ppermute(last0, SLAB, up)
    sent = call(resend_kernel, [RAY], [*parts, weights])[0]
    late = (*parts, sent)
    pieces = to_everyone(sent)
    pieces, first0, last0 = lax.optimization_barrier((pieces, first0, last0))

    mine, theirs, back, crossed, first, last = call(
        third_kernel,
        [half, half, field, (2, 8, 128), (16, 8, 128), (16, 8, 128)],
        [*spots, plain, turned, *pieces, grad],
        scratch,
        3,
    )
    p0, curve0, spare = call(middle_kernel, [RAY, tile, field], [*late, back])
    parts = summed_by_owner(mine, theirs)
    first, last = lax.ppermute(first, SLAB, down), lax.ppermute(last, SLAB, up)
    everyone = slabs * lax.axis_size(TILE)
    q0, rows = call(
        end_kernel, [RAY, (everyone, 128)], [*parts, weights, p0, norm0, curve0, crossed]
    )
    rows, ends = lax.optimization_barrier((rows, ends))
    rows = over_all(rows)
    alphas, again = pl.pallas_call(
        judge_kernel,
        out_shape=[jax.ShapeDtypeStruct((2,), F32), jax.ShapeDtypeStruct((1,), jnp.int32)],
        in_specs=[VM],
        out_specs=[SM, SM],
        compiler_params=pltpu.CompilerParams(vmem_limit_bytes=8 << 20),
    )(rows)

    def summed_again(alphas):
        rows = call(again_kernel, [(everyone, 128)], [alphas, weights, p0, q0, grad, spare], (), 1)[0]
        return pl.pallas_call(
            ratio_kernel,
            out_shape=jax.ShapeDtypeStruct((2,), F32),
            in_specs=[SM, VM],
            out_specs=SM,
            compiler_params=pltpu.CompilerParams(vmem_limit_bytes=8 << 20),
        )(alphas, over_all(rows))

    alphas = lax.cond(again[0] == 1, summed_again, lambda known: known, alphas)
    return call(
        smooth_kernel,
        [volume.shape, measured.shape],
        [ends, alphas, volume, grad, back, first0, last0, first, last, residual, p0, q0],
        (),
        2,
    )


def solution(mesh):
    finer = Mesh(mesh.devices.reshape(4, 2, 4, 4), ("tile_0", "tile_1", "slab_0", "slab_1"))
    return jax.shard_map(
        lambda *args: tuple(shards(*args)),
        mesh=finer,
        in_specs=(
            P(SLAB, TILE),
            P(SLAB, TILE),
            P(SLAB, TILE),
            P(TILE, None, None),
            P(TILE),
            P(TILE),
        ),
        out_specs=(P(SLAB, TILE), P(SLAB, TILE)),
        check_vma=False,
    )
```

```python
import jax
import jax.numpy as jnp
from jax import lax
from jax.experimental import pallas as pl
from jax.experimental.pallas import tpu as pltpu
from jax.sharding import Mesh
from jax.sharding import PartitionSpec as P


PASSES = 3
TILE = ("tile_0", "tile_1")
SLAB = ("slab_0", "slab_1")
GROUP = 4
UNROLL = 32
CHUNKS = 4

huber_width = 0.5
smooth_rate = 0.2


VM = pl.BlockSpec(memory_space=pltpu.VMEM)
SM = pl.BlockSpec(memory_space=pltpu.SMEM)
AN = pl.BlockSpec(memory_space=pltpu.HBM)
F32 = jnp.float32
BF16 = jnp.bfloat16


def call(kernel, outs, ins, scratch=(), smem=0, flops=1000000, limit=10, any_at=()):
    specs = [AN if n in any_at else SM if n < smem else VM for n in range(len(ins))]
    return pl.pallas_call(
        kernel,
        out_shape=[s if hasattr(s, "dtype") else jax.ShapeDtypeStruct(s, F32) for s in outs],
        in_specs=specs,
        out_specs=[VM] * len(outs),
        scratch_shapes=list(scratch),
        compiler_params=pltpu.CompilerParams(vmem_limit_bytes=limit << 20),
        cost_estimate=pl.CostEstimate(flops=flops, bytes_accessed=1 << 20, transcendentals=0),
    )(*ins)


def halves(value):
    high = value.astype(BF16)
    return high, (value - high.astype(F32)).astype(BF16)


def lane_groups(shape):
    return lax.broadcasted_iota(jnp.int32, shape, 1) // 32


def place(spots, b):
    pixels, strips, me = spots
    strip = strips[b]
    owner = strip >> 5
    slot = (((owner & 1) ^ me[1]) << 2) | (((owner >> 1) - me[0]) & 3)
    return (slot << 3) | ((strip >> 2) & 7), strip & 3, pixels[b]


def stacked(pair):
    high = pair[:, :128]
    return jnp.concatenate([pair, jnp.concatenate([high, jnp.zeros_like(high)], axis=1)], axis=0)


def forward_step(spots, g, pair, high, low, rays, groups):
    where = [place(spots, GROUP * g + i) for i in range(GROUP)]
    left = jnp.concatenate([jnp.concatenate([high[w[2]], low[w[2]]], axis=1) for w in where], axis=0)
    both = lax.dot_general(left, stacked(pair), (((1,), (0,)), ((), ())), preferred_element_type=F32)
    product = both[:, :128] + both[:, 128:]
    for i, (entry, spot, _) in enumerate(where):
        own = jnp.where(groups == i, product[32 * i : 32 * i + 32], 0.0)
        rays[entry] += pltpu.roll(own, ((spot - i) & 3) * 32, 1)


def forward_loop(spots, turned, high, low, rays):
    rays[...] = jnp.zeros_like(rays)
    groups = lane_groups((32, 128))

    def step(g, carry):
        forward_step(spots, g, turned[g], high, low, rays, groups)
        return carry

    lax.fori_loop(0, turned.shape[0], step, 0, unroll=UNROLL)


def back_loop(spots, plain, rays, field):
    field[...] = jnp.zeros_like(field)
    groups = lane_groups((32, 128))

    def step(g, carry):
        where = [place(spots, GROUP * g + i) for i in range(GROUP)]
        rows = []
        for i, (entry, spot, _) in enumerate(where):
            turned = pltpu.roll(rays[entry], ((i - spot) & 3) * 32, 1)
            own = jnp.where(groups == i, turned, 0.0)
            rows.append(jnp.concatenate(halves(own), axis=1))
        left = jnp.concatenate(rows, axis=0)
        both = lax.dot_general(
            left, stacked(plain[g]), (((1,), (0,)), ((), ())), preferred_element_type=F32
        )
        product = both[:, :128] + both[:, 128:]
        for i, (_, _, pixel) in enumerate(where):
            field[pixel] += product[32 * i : 32 * i + 32]
        return carry

    lax.fori_loop(0, plain.shape[0], step, 0, unroll=UNROLL)


def hand_out(rays, mine, theirs):
    mine[...] = rays[:32].reshape(mine.shape)
    theirs[...] = rays[32:].reshape(theirs.shape)


def first_kernel(pixels_hbm, strips_hbm, me, foot_hbm, volume_hbm, *refs):
    mine, theirs, first, last, plain, turned, foot, volume, high, low, rays, pixels, strips, sem, foot_sem = refs
    spots = (pixels, strips, me)
    per = foot.shape[0] // CHUNKS

    def chunk(t):
        some = pl.ds(t * per, per)
        return pltpu.make_async_copy(foot_hbm.at[some], foot.at[some], foot_sem.at[t])

    field = pltpu.make_async_copy(volume_hbm, volume, sem.at[0])
    field.start()
    indices = [
        pltpu.make_async_copy(pixels_hbm, pixels, sem.at[1]),
        pltpu.make_async_copy(strips_hbm, strips, sem.at[2]),
    ]
    for copy in indices:
        copy.start()
    for t in range(CHUNKS):
        chunk(t).start()
    rays[...] = jnp.zeros_like(rays)
    groups = lane_groups((32, 128))
    for copy in (*indices, field):
        copy.wait()
    for p in range(high.shape[0]):
        cols = slice(128 * p, 128 * p + 128)
        high[p], low[p] = halves(volume[:, cols])
        first[p], last[p] = volume[0:8, cols], volume[24:32, cols]

    def trip(t, carry):
        chunk(t).wait()
        for u in range(per // GROUP):
            g = t * (per // GROUP) + u
            block = foot[pl.ds(GROUP * g, GROUP)].reshape(GROUP * 32, 128)
            plain[g] = jnp.concatenate(halves(block), axis=1)
            pair = jnp.concatenate(halves(block.T), axis=1)
            turned[g] = pair
            forward_step(spots, g, pair, high, low, rays, groups)
        return carry

    lax.fori_loop(0, CHUNKS, trip, 0)
    hand_out(rays, mine, theirs)


def folded(value):
    return jnp.sum(value.reshape(-1, 8, 128), axis=0)


def there_and_back(spots, plain, turned, pieces, mine, theirs, field, high, low, rays):
    for slot, piece in enumerate(pieces):
        rays[8 * slot : 8 * slot + 8] = piece[...]
    back_loop(spots, plain, rays, field)
    for p in range(high.shape[0]):
        high[p], low[p] = halves(field[p])
    forward_loop(spots, turned, high, low, rays)
    hand_out(rays, mine, theirs)


def two_firsts(one, other):
    row = lax.broadcasted_iota(jnp.int32, (8, 128), 0)
    return jnp.where(row < 3, one, pltpu.roll(other, 3, 0))


def two_lasts(one, other):
    row = lax.broadcasted_iota(jnp.int32, (8, 128), 0)
    return jnp.where(row > 4, one, pltpu.roll(other, 5, 0))


def second_kernel(pixels, strips, me, plain, turned, *refs):
    pieces, first0, last0 = refs[:8], refs[8], refs[9]
    mine, theirs, field, sums, first, last, high, low, rays = refs[10:]
    there_and_back((pixels, strips, me), plain, turned, pieces, mine, theirs, field, high, low, rays)
    sums[0] = folded(field[...] * field[...])
    for p in range(field.shape[0]):
        first[p] = two_firsts(first0[p], field[p, 0:8])
        last[p] = two_lasts(last0[p], field[p, 24:32])


def third_kernel(pixels, strips, me, plain, turned, *refs):
    pieces, grad = refs[:8], refs[8]
    mine, theirs, field, sums, first, last, high, low, rays = refs[9:]
    there_and_back((pixels, strips, me), plain, turned, pieces, mine, theirs, field, high, low, rays)
    sums[0] = folded(grad[...] * field[...])
    sums[1] = folded(field[...] * field[...])
    for q in range(first.shape[0]):
        one, other = field[2 * q], field[2 * q + 1]
        first[q] = two_firsts(one[0:8], other[0:8])
        last[q] = two_lasts(one[24:32], other[24:32])


def add_kernel(mine, got, kept, s1, s2, s3):
    for r, out in enumerate((kept, s1, s2, s3)):
        out[...] = mine[r] + got[r]


def tile_cols(ref):
    return jnp.stack([ref[:, 128 * t : 128 * t + 128] for t in range(ref.shape[1] // 128)])


def start_kernel(kept, a, b, c, measured, weights, residual, sent):
    value = kept[...] + a[...] + b[...] + c[...] - tile_cols(measured)
    residual[...] = value
    sent[...] = tile_cols(weights) * value


def resend_kernel(kept, a, b, c, weights, sent):
    sent[...] = tile_cols(weights) * (kept[...] + a[...] + b[...] + c[...])


def middle_kernel(kept, a, b, c, sent, back, projected, sums, spare):
    spare[...] = back[...]
    value = kept[...] + a[...] + b[...] + c[...]
    projected[...] = value
    sums[0] = folded(sent[...] * value)


SPAN = 16


def in_lanes(sums, shape):
    rows = [jnp.sum(part, axis=0, keepdims=True) for part in sums]
    rows += [jnp.zeros((1, 128), F32)] * (8 - len(rows))
    value = jnp.concatenate(rows, axis=0)
    for by in (64, 32, 16):
        value = value + pltpu.roll(value, by, 1)
    own = lax.broadcasted_iota(jnp.int32, (8, 128), 0) == lax.broadcasted_iota(jnp.int32, (8, 128), 1) // SPAN
    return jnp.broadcast_to(jnp.sum(jnp.where(own, value, 0.0), axis=0, keepdims=True), shape)


def end_kernel(kept, a, b, c, weights, before, norm0, curve0, turned, projected, rows):
    value = kept[...] + a[...] + b[...] + c[...]
    weighted = tile_cols(weights) * value
    projected[...] = value
    cross = folded(weighted * before[...])
    rows[...] = in_lanes([norm0[0], curve0[0], turned[0], turned[1], cross, folded(weighted * value)], rows.shape)


def totals(rows, count):
    value = jnp.sum(rows[...], axis=0, keepdims=True)
    group = lax.broadcasted_iota(jnp.int32, value.shape, 1) // SPAN
    return [jnp.sum(jnp.where(group == n, value, 0.0), axis=1, keepdims=True) for n in range(count)]


def scalar(value):
    return jnp.sum(value)


def judge_kernel(rows, alphas, again):
    norm0, curve0, cross_g, square_g, cross_p, square_p = totals(rows, 6)
    alpha = norm0 / curve0
    norm1 = norm0 - 2.0 * alpha * cross_g + alpha * alpha * square_g
    curve1 = curve0 - 2.0 * alpha * cross_p + alpha * alpha * square_p
    sound = (norm1 > 0.01 * norm0) & (curve1 > 0.01 * curve0)
    for square in (square_g, square_p):
        sound = sound & (square > 1e-25) & (square < 1e37)
    alphas[0] = scalar(alpha)
    alphas[1] = scalar(norm1 / curve1)
    again[0] = jnp.where(scalar(jnp.where(sound, F32(0.0), F32(1.0))) > 0.5, 1, 0)


def again_kernel(alphas, weights, p0, q0, grad, turned, rows):
    value = p0[...] - alphas[0] * q0[...]
    step = grad[...] - alphas[0] * turned[...]
    rows[...] = in_lanes([folded(step * step), folded(tile_cols(weights) * value * value)], rows.shape)


def ratio_kernel(alphas, rows, out):
    norm1, curve1 = totals(rows, 2)
    out[0] = alphas[0]
    out[1] = scalar(norm1 / curve1)


def smooth_kernel(ends, alphas, volume, grad, turned, first0, last0, first, last, residual, p0, q0, smoothed, left_over):
    alpha0, alpha1 = alphas[0], alphas[1]
    rest = residual[...] - alpha0 * p0[...] - alpha1 * (p0[...] - alpha0 * q0[...])
    for t in range(rest.shape[0]):
        left_over[:, 128 * t : 128 * t + 128] = rest[t]

    def stepped(x, g, h):
        return x - alpha0 * g - alpha1 * (g - alpha0 * h)

    row = lax.broadcasted_iota(jnp.int32, (48, 128), 0)
    open_link = ~(((row == 7) & (ends[0] == 1)) | ((row == 39) & (ends[1] == 1)))
    link = jnp.where(open_link, F32(1.0), F32(0.0))
    for p in range(grad.shape[0]):
        cols = slice(128 * p, 128 * p + 128)
        last_h, first_h = last[p // 2], first[p // 2]
        if p % 2:
            last_h, first_h = pltpu.roll(last_h, 3, 0), pltpu.roll(first_h, 5, 0)
        ext = jnp.concatenate(
            [
                stepped(last0[p], pltpu.roll(last0[p], 3, 0), last_h),
                stepped(volume[:, cols], grad[p], turned[p]),
                stepped(first0[p], pltpu.roll(first0[p], 5, 0), first_h),
            ],
            axis=0,
        )
        for _ in range(PASSES):
            clipped = jnp.clip(pltpu.roll(ext, 47, 0) - ext, -huber_width, huber_width) * link
            ext = ext + smooth_rate * (clipped - pltpu.roll(clipped, 1, 0))
        smoothed[:, cols] = ext[8:40]


def shift(value, axis, by):
    n = lax.axis_size(axis)
    return lax.ppermute(value, axis, [(i, (i + by) % n) for i in range(n)])


RAY = (8, 32, 128)


def summed_by_owner(mine, theirs):
    got = shift(theirs, "tile_1", 1)
    kept, s1, s2, s3 = call(add_kernel, [RAY] * 4, [mine, got])
    moved = []
    for r, part in enumerate((s1, s2, s3), 1):
        moved.append(shift(part, "tile_0", r))
    return kept, *moved


def to_everyone(own):
    column = [own] + [shift(own, "tile_0", -r) for r in (1, 2, 3)]
    return column + [shift(block, "tile_1", 1) for block in column]


def over_all(rows):
    return lax.all_to_all(rows, TILE + SLAB, 0, 0, tiled=True)


def shards(volume, measured, weights, footprints, foot_pixel, foot_strip):
    me = jnp.stack([lax.axis_index("tile_0"), lax.axis_index("tile_1")])
    spots = [foot_pixel, foot_strip, me]
    slabs = lax.axis_size(SLAB)
    place_in = lax.axis_index(SLAB)
    ends = jnp.stack([place_in == 0, place_in == slabs - 1]).astype(jnp.int32)
    up = [(i, (i + 1) % slabs) for i in range(slabs)]
    down = [(j, i) for i, j in up]

    field, tile = (32, 32, 128), (1, 8, 128)
    scratch = [pltpu.VMEM(field, BF16), pltpu.VMEM(field, BF16), pltpu.VMEM((64, 32, 128), F32)]
    in_place = [pltpu.with_memory_space_constraint(x, pltpu.HBM) for x in (foot_pixel, foot_strip, footprints, volume)]
    streams = [
        pltpu.VMEM(footprints.shape, F32),
        pltpu.VMEM(volume.shape, F32),
        *scratch,
        pltpu.SMEM(foot_pixel.shape, jnp.int32),
        pltpu.SMEM(foot_strip.shape, jnp.int32),
        pltpu.SemaphoreType.DMA((3,)),
        pltpu.SemaphoreType.DMA((CHUNKS,)),
    ]
    split = jax.ShapeDtypeStruct((64, 128, 256), BF16)
    half, edge = (4,) + RAY, (32, 8, 128)
    mine, theirs, first0, last0, plain, turned = call(
        first_kernel,
        [half, half, edge, edge, split, split],
        [*in_place[:2], me, *in_place[2:]],
        streams,
        3,
        any_at=(0, 1, 3, 4),
        limit=16,
    )
    parts = summed_by_owner(mine, theirs)
    residual, sent = call(start_kernel, [RAY, RAY], [*parts, measured, weights])

    mine, theirs, grad, norm0, first0, last0 = call(
        second_kernel,
        [half, half, field, tile, edge, edge],
        [*spots, plain, turned, *to_everyone(sent), first0, last0],
        scratch,
        3,
    )
    parts = summed_by_owner(mine, theirs)
    first0, last0 = lax.ppermute(first0, SLAB, down), lax.ppermute(last0, SLAB, up)
    sent = call(resend_kernel, [RAY], [*parts, weights])[0]
    late = (*parts, sent)
    pieces = to_everyone(sent)
    pieces, first0, last0 = lax.optimization_barrier((pieces, first0, last0))

    mine, theirs, back, crossed, first, last = call(
        third_kernel,
        [half, half, field, (2, 8, 128), (16, 8, 128), (16, 8, 128)],
        [*spots, plain, turned, *pieces, grad],
        scratch,
        3,
    )
    p0, curve0, spare = call(middle_kernel, [RAY, tile, field], [*late, back])
    parts = summed_by_owner(mine, theirs)
    first, last = lax.ppermute(first, SLAB, down), lax.ppermute(last, SLAB, up)
    everyone = slabs * lax.axis_size(TILE)
    q0, rows = call(
        end_kernel, [RAY, (everyone, 128)], [*parts, weights, p0, norm0, curve0, crossed]
    )
    rows, ends = lax.optimization_barrier((rows, ends))
    rows = over_all(rows)
    alphas, again = pl.pallas_call(
        judge_kernel,
        out_shape=[jax.ShapeDtypeStruct((2,), F32), jax.ShapeDtypeStruct((1,), jnp.int32)],
        in_specs=[VM],
        out_specs=[SM, SM],
        compiler_params=pltpu.CompilerParams(vmem_limit_bytes=8 << 20),
    )(rows)

    def summed_again(alphas):
        rows = call(again_kernel, [(everyone, 128)], [alphas, weights, p0, q0, grad, spare], (), 1)[0]
        return pl.pallas_call(
            ratio_kernel,
            out_shape=jax.ShapeDtypeStruct((2,), F32),
            in_specs=[SM, VM],
            out_specs=SM,
            compiler_params=pltpu.CompilerParams(vmem_limit_bytes=8 << 20),
        )(alphas, over_all(rows))

    alphas = lax.cond(again[0] == 1, summed_again, lambda known: known, alphas)
    return call(
        smooth_kernel,
        [volume.shape, measured.shape],
        [ends, alphas, volume, grad, back, first0, last0, first, last, residual, p0, q0],
        (),
        2,
    )


def solution(mesh):
    finer = Mesh(mesh.devices.reshape(4, 2, 4, 4), ("tile_0", "tile_1", "slab_0", "slab_1"))
    return jax.shard_map(
        lambda *args: tuple(shards(*args)),
        mesh=finer,
        in_specs=(
            P(SLAB, TILE),
            P(SLAB, TILE),
            P(SLAB, TILE),
            P(TILE, None, None),
            P(TILE),
            P(TILE),
        ),
        out_specs=(P(SLAB, TILE), P(SLAB, TILE)),
        check_vma=False,
    )
```

```python
import jax
import jax.numpy as jnp
from jax import lax
from jax.experimental import pallas as pl
from jax.experimental.pallas import tpu as pltpu
from jax.sharding import Mesh
from jax.sharding import PartitionSpec as P


PASSES = 3
TILE = ("tile_0", "tile_1")
SLAB = ("slab_0", "slab_1")
GROUP = 4
UNROLL = 32
CHUNKS = 4

huber_width = 0.5
smooth_rate = 0.2


VM = pl.BlockSpec(memory_space=pltpu.VMEM)
SM = pl.BlockSpec(memory_space=pltpu.SMEM)
AN = pl.BlockSpec(memory_space=pltpu.HBM)
F32 = jnp.float32
BF16 = jnp.bfloat16


def call(kernel, outs, ins, scratch=(), smem=0, flops=1000000, limit=10, any_at=()):
    specs = [AN if n in any_at else SM if n < smem else VM for n in range(len(ins))]
    return pl.pallas_call(
        kernel,
        out_shape=[s if hasattr(s, "dtype") else jax.ShapeDtypeStruct(s, F32) for s in outs],
        in_specs=specs,
        out_specs=[VM] * len(outs),
        scratch_shapes=list(scratch),
        compiler_params=pltpu.CompilerParams(vmem_limit_bytes=limit << 20),
        cost_estimate=pl.CostEstimate(flops=flops, bytes_accessed=1 << 20, transcendentals=0),
    )(*ins)


def halves(value):
    high = value.astype(BF16)
    return high, (value - high.astype(F32)).astype(BF16)


def lane_groups(shape):
    return lax.broadcasted_iota(jnp.int32, shape, 1) // 32


def place(spots, b):
    pixels, strips, me = spots
    strip = strips[b]
    owner = strip >> 5
    slot = (((owner & 1) ^ me[1]) << 2) | (((owner >> 1) - me[0]) & 3)
    return (slot << 3) | ((strip >> 2) & 7), strip & 3, pixels[b]


def stacked(pair):
    high = pair[:, :128]
    return jnp.concatenate([pair, jnp.concatenate([high, jnp.zeros_like(high)], axis=1)], axis=0)


def forward_step(spots, g, pair, high, low, rays, groups):
    where = [place(spots, GROUP * g + i) for i in range(GROUP)]
    left = jnp.concatenate([jnp.concatenate([high[w[2]], low[w[2]]], axis=1) for w in where], axis=0)
    both = lax.dot_general(left, stacked(pair), (((1,), (0,)), ((), ())), preferred_element_type=F32)
    product = both[:, :128] + both[:, 128:]
    for i, (entry, spot, _) in enumerate(where):
        own = jnp.where(groups == i, product[32 * i : 32 * i + 32], 0.0)
        rays[entry] += pltpu.roll(own, ((spot - i) & 3) * 32, 1)


def forward_loop(spots, turned, high, low, rays):
    rays[...] = jnp.zeros_like(rays)
    groups = lane_groups((32, 128))

    def step(g, carry):
        forward_step(spots, g, turned[g], high, low, rays, groups)
        return carry

    lax.fori_loop(0, turned.shape[0], step, 0, unroll=UNROLL)


def back_loop(spots, plain, rays, field):
    field[...] = jnp.zeros_like(field)
    groups = lane_groups((32, 128))

    def step(g, carry):
        where = [place(spots, GROUP * g + i) for i in range(GROUP)]
        rows = []
        for i, (entry, spot, _) in enumerate(where):
            turned = pltpu.roll(rays[entry], ((i - spot) & 3) * 32, 1)
            own = jnp.where(groups == i, turned, 0.0)
            rows.append(jnp.concatenate(halves(own), axis=1))
        left = jnp.concatenate(rows, axis=0)
        both = lax.dot_general(
            left, stacked(plain[g]), (((1,), (0,)), ((), ())), preferred_element_type=F32
        )
        product = both[:, :128] + both[:, 128:]
        for i, (_, _, pixel) in enumerate(where):
            field[pixel] += product[32 * i : 32 * i + 32]
        return carry

    lax.fori_loop(0, plain.shape[0], step, 0, unroll=UNROLL)


def hand_out(rays, mine, theirs):
    mine[...] = rays[:32].reshape(mine.shape)
    theirs[...] = rays[32:].reshape(theirs.shape)


def first_kernel(pixels_hbm, strips_hbm, me, foot_hbm, volume_hbm, *refs):
    mine, theirs, first, last, plain, turned, foot, volume, high, low, rays, pixels, strips, sem, foot_sem = refs
    spots = (pixels, strips, me)
    per = foot.shape[0] // CHUNKS

    def chunk(t):
        some = pl.ds(t * per, per)
        return pltpu.make_async_copy(foot_hbm.at[some], foot.at[some], foot_sem.at[t])

    field = pltpu.make_async_copy(volume_hbm, volume, sem.at[0])
    field.start()
    indices = [
        pltpu.make_async_copy(pixels_hbm, pixels, sem.at[1]),
        pltpu.make_async_copy(strips_hbm, strips, sem.at[2]),
    ]
    for copy in indices:
        copy.start()
    for t in range(CHUNKS):
        chunk(t).start()
    rays[...] = jnp.zeros_like(rays)
    groups = lane_groups((32, 128))
    for copy in (*indices, field):
        copy.wait()
    for p in range(high.shape[0]):
        cols = slice(128 * p, 128 * p + 128)
        high[p], low[p] = halves(volume[:, cols])
        first[p], last[p] = volume[0:8, cols], volume[24:32, cols]

    def trip(t, carry):
        chunk(t).wait()
        for u in range(per // GROUP):
            g = t * (per // GROUP) + u
            block = foot[pl.ds(GROUP * g, GROUP)].reshape(GROUP * 32, 128)
            plain[g] = jnp.concatenate(halves(block), axis=1)
            pair = jnp.concatenate(halves(block.T), axis=1)
            turned[g] = pair
            forward_step(spots, g, pair, high, low, rays, groups)
        return carry

    lax.fori_loop(0, CHUNKS, trip, 0)
    hand_out(rays, mine, theirs)


def folded(value):
    return jnp.sum(value.reshape(-1, 8, 128), axis=0)


def there_and_back(spots, plain, turned, pieces, mine, theirs, field, high, low, rays):
    for slot, piece in enumerate(pieces):
        rays[8 * slot : 8 * slot + 8] = piece[...]
    back_loop(spots, plain, rays, field)
    for p in range(high.shape[0]):
        high[p], low[p] = halves(field[p])
    forward_loop(spots, turned, high, low, rays)
    hand_out(rays, mine, theirs)


def two_firsts(one, other):
    row = lax.broadcasted_iota(jnp.int32, (8, 128), 0)
    return jnp.where(row < 3, one, pltpu.roll(other, 3, 0))


def two_lasts(one, other):
    row = lax.broadcasted_iota(jnp.int32, (8, 128), 0)
    return jnp.where(row > 4, one, pltpu.roll(other, 5, 0))


def second_kernel(pixels, strips, me, plain, turned, *refs):
    pieces, first0, last0 = refs[:8], refs[8], refs[9]
    mine, theirs, field, sums, first, last, high, low, rays = refs[10:]
    there_and_back((pixels, strips, me), plain, turned, pieces, mine, theirs, field, high, low, rays)
    sums[0] = folded(field[...] * field[...])
    for p in range(field.shape[0]):
        first[p] = two_firsts(first0[p], field[p, 0:8])
        last[p] = two_lasts(last0[p], field[p, 24:32])


def third_kernel(pixels, strips, me, plain, turned, *refs):
    pieces, grad = refs[:8], refs[8]
    mine, theirs, field, sums, first, last, high, low, rays = refs[9:]
    there_and_back((pixels, strips, me), plain, turned, pieces, mine, theirs, field, high, low, rays)
    sums[0] = folded(grad[...] * field[...])
    sums[1] = folded(field[...] * field[...])
    for q in range(first.shape[0]):
        one, other = field[2 * q], field[2 * q + 1]
        first[q] = two_firsts(one[0:8], other[0:8])
        last[q] = two_lasts(one[24:32], other[24:32])


def add_kernel(mine, got, kept, s1, s2, s3):
    for r, out in enumerate((kept, s1, s2, s3)):
        out[...] = mine[r] + got[r]


def tile_cols(ref):
    return jnp.stack([ref[:, 128 * t : 128 * t + 128] for t in range(ref.shape[1] // 128)])


def start_kernel(kept, a, b, c, measured, weights, residual, sent):
    value = kept[...] + a[...] + b[...] + c[...] - tile_cols(measured)
    residual[...] = value
    sent[...] = tile_cols(weights) * value


def resend_kernel(kept, a, b, c, weights, sent):
    sent[...] = tile_cols(weights) * (kept[...] + a[...] + b[...] + c[...])


def middle_kernel(kept, a, b, c, sent, back, projected, sums, spare):
    spare[...] = back[...]
    value = kept[...] + a[...] + b[...] + c[...]
    projected[...] = value
    sums[0] = folded(sent[...] * value)


SPAN = 16


def in_lanes(sums, shape):
    rows = [jnp.sum(part, axis=0, keepdims=True) for part in sums]
    rows += [jnp.zeros((1, 128), F32)] * (8 - len(rows))
    value = jnp.concatenate(rows, axis=0)
    for by in (64, 32, 16):
        value = value + pltpu.roll(value, by, 1)
    own = lax.broadcasted_iota(jnp.int32, (8, 128), 0) == lax.broadcasted_iota(jnp.int32, (8, 128), 1) // SPAN
    return jnp.broadcast_to(jnp.sum(jnp.where(own, value, 0.0), axis=0, keepdims=True), shape)


def end_kernel(kept, a, b, c, weights, before, norm0, curve0, turned, projected, rows):
    value = kept[...] + a[...] + b[...] + c[...]
    weighted = tile_cols(weights) * value
    projected[...] = value
    cross = folded(weighted * before[...])
    rows[...] = in_lanes([norm0[0], curve0[0], turned[0], turned[1], cross, folded(weighted * value)], rows.shape)


def totals(rows, count):
    value = jnp.sum(rows[...], axis=0, keepdims=True)
    group = lax.broadcasted_iota(jnp.int32, value.shape, 1) // SPAN
    return [jnp.sum(jnp.where(group == n, value, 0.0), axis=1, keepdims=True) for n in range(count)]


def scalar(value):
    return jnp.sum(value)


def judge_kernel(rows, alphas, again):
    norm0, curve0, cross_g, square_g, cross_p, square_p = totals(rows, 6)
    alpha = norm0 / curve0
    norm1 = norm0 - 2.0 * alpha * cross_g + alpha * alpha * square_g
    curve1 = curve0 - 2.0 * alpha * cross_p + alpha * alpha * square_p
    sound = (norm1 > 0.01 * norm0) & (curve1 > 0.01 * curve0)
    for square in (square_g, square_p):
        sound = sound & (square > 1e-25) & (square < 1e37)
    alphas[0] = scalar(alpha)
    alphas[1] = scalar(norm1 / curve1)
    again[0] = jnp.where(scalar(jnp.where(sound, F32(0.0), F32(1.0))) > 0.5, 1, 0)


def again_kernel(alphas, weights, p0, q0, grad, turned, rows):
    value = p0[...] - alphas[0] * q0[...]
    step = grad[...] - alphas[0] * turned[...]
    rows[...] = in_lanes([folded(step * step), folded(tile_cols(weights) * value * value)], rows.shape)


def ratio_kernel(alphas, rows, out):
    norm1, curve1 = totals(rows, 2)
    out[0] = alphas[0]
    out[1] = scalar(norm1 / curve1)


def smooth_kernel(ends, alphas, volume, grad, turned, first0, last0, first, last, residual, p0, q0, smoothed, left_over):
    alpha0, alpha1 = alphas[0], alphas[1]
    rest = residual[...] - alpha0 * p0[...] - alpha1 * (p0[...] - alpha0 * q0[...])
    for t in range(rest.shape[0]):
        left_over[:, 128 * t : 128 * t + 128] = rest[t]

    def stepped(x, g, h):
        return x - alpha0 * g - alpha1 * (g - alpha0 * h)

    row = lax.broadcasted_iota(jnp.int32, (48, 128), 0)
    open_link = ~(((row == 7) & (ends[0] == 1)) | ((row == 39) & (ends[1] == 1)))
    link = jnp.where(open_link, F32(1.0), F32(0.0))
    for p in range(grad.shape[0]):
        cols = slice(128 * p, 128 * p + 128)
        last_h, first_h = last[p // 2], first[p // 2]
        if p % 2:
            last_h, first_h = pltpu.roll(last_h, 3, 0), pltpu.roll(first_h, 5, 0)
        ext = jnp.concatenate(
            [
                stepped(last0[p], pltpu.roll(last0[p], 3, 0), last_h),
                stepped(volume[:, cols], grad[p], turned[p]),
                stepped(first0[p], pltpu.roll(first0[p], 5, 0), first_h),
            ],
            axis=0,
        )
        for _ in range(PASSES):
            clipped = jnp.clip(pltpu.roll(ext, 47, 0) - ext, -huber_width, huber_width) * link
            ext = ext + smooth_rate * (clipped - pltpu.roll(clipped, 1, 0))
        smoothed[:, cols] = ext[8:40]


def shift(value, axis, by):
    n = lax.axis_size(axis)
    return lax.ppermute(value, axis, [(i, (i + by) % n) for i in range(n)])


RAY = (8, 32, 128)


def summed_by_owner(mine, theirs):
    got = shift(theirs, "tile_1", 1)
    kept, s1, s2, s3 = call(add_kernel, [RAY] * 4, [mine, got])
    moved = []
    for r, part in enumerate((s1, s2, s3), 1):
        moved.append(shift(part, "tile_0", r))
    return kept, *moved


def to_everyone(own):
    column = [own]
    for r in (1, 2, 3):
        column.append(shift(own, "tile_0", -r))
    return column + [shift(block, "tile_1", 1) for block in column]


def over_all(rows):
    return lax.all_to_all(rows, TILE + SLAB, 0, 0, tiled=True)


def shards(volume, measured, weights, footprints, foot_pixel, foot_strip):
    me = jnp.stack([lax.axis_index("tile_0"), lax.axis_index("tile_1")])
    spots = [foot_pixel, foot_strip, me]
    slabs = lax.axis_size(SLAB)
    place_in = lax.axis_index(SLAB)
    ends = jnp.stack([place_in == 0, place_in == slabs - 1]).astype(jnp.int32)
    up = [(i, (i + 1) % slabs) for i in range(slabs)]
    down = [(j, i) for i, j in up]

    field, tile = (32, 32, 128), (1, 8, 128)
    scratch = [pltpu.VMEM(field, BF16), pltpu.VMEM(field, BF16), pltpu.VMEM((64, 32, 128), F32)]
    in_place = [pltpu.with_memory_space_constraint(x, pltpu.HBM) for x in (foot_pixel, foot_strip, footprints, volume)]
    streams = [
        pltpu.VMEM(footprints.shape, F32),
        pltpu.VMEM(volume.shape, F32),
        *scratch,
        pltpu.SMEM(foot_pixel.shape, jnp.int32),
        pltpu.SMEM(foot_strip.shape, jnp.int32),
        pltpu.SemaphoreType.DMA((3,)),
        pltpu.SemaphoreType.DMA((CHUNKS,)),
    ]
    split = jax.ShapeDtypeStruct((64, 128, 256), BF16)
    half, edge = (4,) + RAY, (32, 8, 128)
    mine, theirs, first0, last0, plain, turned = call(
        first_kernel,
        [half, half, edge, edge, split, split],
        [*in_place[:2], me, *in_place[2:]],
        streams,
        3,
        any_at=(0, 1, 3, 4),
        limit=16,
    )
    parts = summed_by_owner(mine, theirs)
    residual, sent = call(start_kernel, [RAY, RAY], [*parts, measured, weights])

    pieces = to_everyone(sent)
    mine, theirs, grad, norm0, first0, last0 = call(
        second_kernel,
        [half, half, field, tile, edge, edge],
        [*spots, plain, turned, *pieces, first0, last0],
        scratch,
        3,
    )
    parts = summed_by_owner(mine, theirs)
    first0, last0 = lax.ppermute(first0, SLAB, down), lax.ppermute(last0, SLAB, up)
    sent = call(resend_kernel, [RAY], [*parts, weights])[0]
    late = (*parts, sent)
    pieces = to_everyone(sent)
    pieces, first0, last0 = lax.optimization_barrier((pieces, first0, last0))

    mine, theirs, back, crossed, first, last = call(
        third_kernel,
        [half, half, field, (2, 8, 128), (16, 8, 128), (16, 8, 128)],
        [*spots, plain, turned, *pieces, grad],
        scratch,
        3,
    )
    p0, curve0, spare = call(middle_kernel, [RAY, tile, field], [*late, back])
    parts = summed_by_owner(mine, theirs)
    first, last = lax.ppermute(first, SLAB, down), lax.ppermute(last, SLAB, up)
    everyone = slabs * lax.axis_size(TILE)
    q0, rows = call(
        end_kernel, [RAY, (everyone, 128)], [*parts, weights, p0, norm0, curve0, crossed]
    )
    rows, ends = lax.optimization_barrier((rows, ends))
    rows = over_all(rows)
    alphas, again = pl.pallas_call(
        judge_kernel,
        out_shape=[jax.ShapeDtypeStruct((2,), F32), jax.ShapeDtypeStruct((1,), jnp.int32)],
        in_specs=[VM],
        out_specs=[SM, SM],
        compiler_params=pltpu.CompilerParams(vmem_limit_bytes=8 << 20),
    )(rows)

    def summed_again(alphas):
        rows = call(again_kernel, [(everyone, 128)], [alphas, weights, p0, q0, grad, spare], (), 1)[0]
        return pl.pallas_call(
            ratio_kernel,
            out_shape=jax.ShapeDtypeStruct((2,), F32),
            in_specs=[SM, VM],
            out_specs=SM,
            compiler_params=pltpu.CompilerParams(vmem_limit_bytes=8 << 20),
        )(alphas, over_all(rows))

    alphas = lax.cond(again[0] == 1, summed_again, lambda known: known, alphas)
    return call(
        smooth_kernel,
        [volume.shape, measured.shape],
        [ends, alphas, volume, grad, back, first0, last0, first, last, residual, p0, q0],
        (),
        2,
    )


def solution(mesh):
    finer = Mesh(mesh.devices.reshape(4, 2, 4, 4), ("tile_0", "tile_1", "slab_0", "slab_1"))
    return jax.shard_map(
        lambda *args: tuple(shards(*args)),
        mesh=finer,
        in_specs=(
            P(SLAB, TILE),
            P(SLAB, TILE),
            P(SLAB, TILE),
            P(TILE, None, None),
            P(TILE),
            P(TILE),
        ),
        out_specs=(P(SLAB, TILE), P(SLAB, TILE)),
        check_vma=False,
    )
```
